64 devices in a mesh: dp: 4 (over x, y), sp: 16 (over z, core).
Axes of the slice: x: 2, y: 2, z: 8, core: 2. Of those that a mesh axis runs over, the one named last changes fastest.
The devices are a block of a 4x4x8 slice.
Arguments:
- tokens: bfloat16 [65536, 1536], P(('dp', 'sp')), parts along dimension 0
- w_q: bfloat16 [1536, 1536], replicated
- w_k: bfloat16 [1536, 1536], replicated
- w_v: bfloat16 [1536, 1536], replicated
- w_o: bfloat16 [1536, 1536], replicated
- grad_y: bfloat16 [65536, 1536], P(('dp', 'sp')), parts along dimension 0
Outputs:
- output 1: bfloat16 [65536, 1536], P(('dp', 'sp')), parts along dimension 0
- output 2: bfloat16 [65536, 1536], P(('dp', 'sp')), parts along dimension 0
- output 3: float32 [6144, 1536], P('dp'), parts along dimension 0
- output 4: float32 [6144, 1536], P('dp'), parts along dimension 0
- output 5: float32 [6144, 1536], P('dp'), parts along dimension 0
- output 6: float32 [6144, 1536], P('dp'), parts along dimension 0
There are 4 independent parts. The reference program is written for one: setup_inputs(seed, part) draws one part's arguments, and reference() takes and returns one part's arrays. A program takes and returns all parts, laid end to end along the dimension named above; an argument that names none is the same for every part.
All inputs are finite; a program needn't handle non-finite values.
Results may differ from the reference program's by a relative error of at most 0.00435663.
Values are sent between devices in bfloat16 or wider.
A program may use at most 768 MiB of HBM per device.

```python
import math
import jax
import jax.numpy as jnp

SEQ_LEN = 16384
MODEL_DIM = 1536
HEAD_DIM = 128
BLOCK_LEN = 128


def setup_inputs(seed: int = 0, part: int = 0) -> dict:
    part_key = jax.random.fold_in(jax.random.key(seed), part)
    key_x, key_dy = jax.random.split(part_key)
    key_q, key_k, key_v, key_o = jax.random.split(jax.random.key(seed + 1), 4)
    w_scale = MODEL_DIM ** -0.5
    shape_w = (MODEL_DIM, MODEL_DIM)

    def normal_weight(key_w):
        return (jax.random.normal(key_w, shape_w, jnp.float32) * w_scale).astype(jnp.bfloat16)

    tokens = jax.random.normal(key_x, (SEQ_LEN, MODEL_DIM), jnp.float32)
    grad_y = jax.random.normal(key_dy, (SEQ_LEN, MODEL_DIM), jnp.float32) * SEQ_LEN ** -0.25
    return {"tokens": tokens.astype(jnp.bfloat16), "w_q": normal_weight(key_q), "w_k": normal_weight(key_k), "w_v": normal_weight(key_v), "w_o": normal_weight(key_o), "grad_y": grad_y.astype(jnp.bfloat16)}


def reference(tokens, w_q, w_k, w_v, w_o, grad_y):
    n_heads = MODEL_DIM // HEAD_DIM
    n_blocks = SEQ_LEN // BLOCK_LEN
    att_scale = 1.0 / math.sqrt(SEQ_LEN * HEAD_DIM)
    causal = jnp.arange(BLOCK_LEN)[:, None] >= jnp.arange(BLOCK_LEN)[None, :]

    def project(operand, weight):
        return jnp.dot(operand, weight, preferred_element_type=jnp.float32).astype(jnp.bfloat16)

    def split_heads(tensor):
        return tensor.reshape(n_blocks, BLOCK_LEN, n_heads, HEAD_DIM).astype(jnp.float32)

    def to_rows(tensor):
        return (tensor * att_scale).astype(jnp.bfloat16).reshape(SEQ_LEN, MODEL_DIM)

    def as_bf16(tensor):
        return tensor.astype(jnp.bfloat16).astype(jnp.float32)

    def excl_prefix(blocks):
        zero_block = jnp.zeros_like(blocks[:1])
        return jnp.concatenate([zero_block, jnp.cumsum(blocks, axis=0)[:-1]], axis=0)

    q_heads = split_heads(project(tokens, w_q))
    k_heads = split_heads(project(tokens, w_k))
    v_heads = split_heads(project(tokens, w_v))
    fwd_state = as_bf16(excl_prefix(jnp.einsum("nshd,nshe->nhde", k_heads, v_heads)))
    masked_scores = as_bf16(jnp.where(causal, jnp.einsum("nthd,nshd->nhts", q_heads, k_heads), 0.0))
    out_rows = to_rows(jnp.einsum("nhts,nshe->nthe", masked_scores, v_heads) + jnp.einsum("nthd,nhde->nthe", q_heads, fwd_state))
    out_y = project(out_rows, w_o)

    do_heads = split_heads(project(grad_y, w_o.T))
    block_qdo = jnp.einsum("nthd,nthe->nhde", q_heads, do_heads)
    rev_state = as_bf16(excl_prefix(block_qdo[::-1])[::-1])
    masked_grads = as_bf16(jnp.where(causal, jnp.einsum("nthe,nshe->nhts", do_heads, v_heads), 0.0))
    dq_rows = to_rows(jnp.einsum("nhts,nshd->nthd", masked_grads, k_heads) + jnp.einsum("nthe,nhde->nthd", do_heads, fwd_state))
    dk_rows = to_rows(jnp.einsum("nhts,nthd->nshd", masked_grads, q_heads) + jnp.einsum("nshe,nhde->nshd", v_heads, rev_state))
    dv_rows = to_rows(jnp.einsum("nhts,nthe->nshe", masked_scores, do_heads) + jnp.einsum("nshd,nhde->nshe", k_heads, rev_state))
    grad_x = (jnp.dot(dq_rows, w_q.T, preferred_element_type=jnp.float32) + jnp.dot(dk_rows, w_k.T, preferred_element_type=jnp.float32) + jnp.dot(dv_rows, w_v.T, preferred_element_type=jnp.float32)).astype(jnp.bfloat16)
    grad_wq = jnp.dot(tokens.T, dq_rows, preferred_element_type=jnp.float32)
    grad_wk = jnp.dot(tokens.T, dk_rows, preferred_element_type=jnp.float32)
    grad_wv = jnp.dot(tokens.T, dv_rows, preferred_element_type=jnp.float32)
    grad_wo = jnp.dot(out_rows.T, grad_y, preferred_element_type=jnp.float32)
    return (out_y, grad_x, grad_wq, grad_wk, grad_wv, grad_wo)
```

```python
import functools
import math
import jax
import jax.numpy as jnp
from jax import lax
from jax.experimental import pallas as pl
from jax.experimental.pallas import tpu as pltpu
from jax.sharding import PartitionSpec as P

HEAD_DIM = 128
BLOCK_LEN = 128
TILE = 128
ROWS = 256
MESH = pl.DeviceIdType.MESH
VMEM_LIMIT = 67_043_328
F32 = jnp.float32
BF16 = jnp.bfloat16


def dot_t(lhs, rhs):
    return lax.dot_general(lhs, rhs, (((0,), (0,)), ((), ())), preferred_element_type=F32)


def dot_nt(lhs, rhs):
    return lax.dot_general(lhs, rhs, (((1,), (1,)), ((), ())), preferred_element_type=F32)


def dot(lhs, rhs):
    return jnp.dot(lhs, rhs, preferred_element_type=F32)


def aligned(index, size):
    return pl.ds(pl.multiple_of(index * size, size), size)


def position(n_seq):
    me = lax.axis_index("sp")
    core, chip = lax.rem(me, 2), lax.div(me, 2)
    return core, chip, n_seq // 2, me + 1 - 2 * core


def send(src, dst, send_sem, recv_sem, target):
    return pltpu.make_async_remote_copy(src_ref=src, dst_ref=dst, send_sem=send_sem, recv_sem=recv_sem, device_id={"sp": target}, device_id_type=MESH)


def entry_barrier(targets):
    barrier = pltpu.get_barrier_semaphore()
    for target in targets:
        pl.semaphore_signal(barrier, inc=1, device_id={"sp": target}, device_id_type=MESH)
    pl.semaphore_wait(barrier, len(targets))


def attention_kernel(n_seq, scale, x, dy, wq, wk, wv, wo, xo_out, ra_out, xf, dyf, w_s, wo_s, q, k, v, do, o, dq, a_s, b_s, kv_s, qdo_s, s_in, s_out, r_in, r_out, x_sems, w_sems, chain_sems, out_sems):
    core, chip, n_chips, peer = position(n_seq)
    me = lax.axis_index("sp")
    up, down = lax.rem(me + 2, n_seq), lax.rem(me + n_seq - 2, n_seq)
    n_rows, dim = x.shape
    all_rows, width = q.shape
    n_heads = width // HEAD_DIM
    n_blocks = all_rows // BLOCK_LEN
    own_rows = aligned(core, n_rows)

    entry_barrier((peer, up, down))
    local = []
    remote = []
    for index, (src, dst) in enumerate(((x, xf), (dy, dyf))):
        remote.append(send(src, dst.at[own_rows], x_sems.at[index, 0], x_sems.at[index, 1], peer))
        local.append(pltpu.make_async_copy(src, dst.at[own_rows], x_sems.at[index, 2]))
    w_cols = aligned(core, width)
    w_loads = [pltpu.make_async_copy(weight.at[:, w_cols], w_s.at[index], w_sems.at[index]) for index, weight in enumerate((wk, wv, wq))]
    w_loads.append(pltpu.make_async_copy(wo.at[w_cols], wo_s, w_sems.at[3]))
    remote[0].start()
    local[0].start()
    for load in w_loads[:2]:
        load.start()
    remote[1].start()
    for load in w_loads[2:]:
        load.start()
    local[1].start()

    def project(half, jobs):
        @pl.loop(0, n_rows // ROWS)
        def _(step):
            rows = pl.ds(pl.multiple_of(half * n_rows + step * ROWS, ROWS), ROWS)
            for src, weight, dst, transposed in jobs:
                product = dot_nt(src[rows, :], weight[...]) if transposed else dot(src[rows, :], weight[...])
                dst[rows, :] = product.astype(BF16)

    kv_jobs = ((xf, w_s.at[0], k, False), (xf, w_s.at[1], v, False))
    qo_jobs = ((xf, w_s.at[2], q, False), (dyf, wo_s, do, True))
    local[0].wait()
    w_loads[0].wait()
    w_loads[1].wait()
    project(core, kv_jobs)
    remote[0].wait()
    project(1 - core, kv_jobs)

    def accumulate(lhs, rhs, kept, total, reverse):
        total[...] = jnp.zeros_like(total)

        @pl.loop(0, n_blocks)
        def _(step):
            block = (n_blocks - 1 - step) if reverse else step
            rows = aligned(block, BLOCK_LEN)
            for h in range(n_heads):
                cols = pl.ds(h * HEAD_DIM, HEAD_DIM)
                running = total[h]
                kept[block, h] = running
                total[h] = running + dot_t(lhs[rows, cols], rhs[rows, cols])

    accumulate(k, v, kv_s, s_out, False)
    local[1].wait()
    w_loads[2].wait()
    w_loads[3].wait()
    project(core, qo_jobs)
    remote[1].wait()
    project(1 - core, qo_jobs)
    accumulate(q, do, qdo_s, r_out, True)

    x_out = pltpu.make_async_copy(xf, xo_out.at[:, pl.ds(0, dim)], out_sems.at[0])
    dy_out = pltpu.make_async_copy(dyf, ra_out.at[:, pl.ds(width, dim)], out_sems.at[1])
    x_out.start()
    dy_out.start()

    def chain_copy(which, h):
        src, dst, target = ((s_out, s_in, up), (r_out, r_in, down))[which]
        return send(src.at[h], dst.at[h], chain_sems.at[which, 0, h], chain_sems.at[which, 1, h], target)

    def chain_step(which, h):
        first, last = ((0, n_chips - 1), (n_chips - 1, 0))[which]
        src, dst = ((s_out, s_in), (r_out, r_in))[which]

        @pl.when(chip == first)
        def _():
            dst[h] = jnp.zeros_like(dst[h])

        @pl.when(chip != first)
        def _():
            chain_copy(which, h).wait_recv()
            src[h] = src[h] + dst[h]

        @pl.when(chip != last)
        def _():
            chain_copy(which, h).start()

    high = lax.div(chip, n_chips // 2)
    lag_s = high * 2 * (2 * chip - (n_chips - 1))
    lag_r = (1 - high) * 2 * ((n_chips - 1) - 2 * chip)

    causal = lax.broadcasted_iota(jnp.int32, (BLOCK_LEN, BLOCK_LEN), 0) >= lax.broadcasted_iota(jnp.int32, (BLOCK_LEN, BLOCK_LEN), 1)

    def block_scores(block):
        rows = aligned(block, BLOCK_LEN)
        for h in range(n_heads):
            cols = pl.ds(h * HEAD_DIM, HEAD_DIM)
            a_s[block, h] = jnp.where(causal, dot_nt(q[rows, cols], k[rows, cols]), 0.0).astype(BF16)
            b_s[block, h] = jnp.where(causal, dot_nt(do[rows, cols], v[rows, cols]), 0.0).astype(BF16)

    @pl.loop(0, max(n_heads + 2 * (n_chips - 1), n_blocks))
    def _(step):
        for which, lag in ((0, lag_s), (1, lag_r)):
            @pl.when((step >= lag) & (step < lag + n_heads))
            def _():
                chain_step(which, step - lag)

        @pl.when(step < n_blocks)
        def _():
            block_scores(step)

    @pl.loop(0, n_blocks)
    def _(block):
        rows = aligned(block, BLOCK_LEN)
        for h in range(n_heads):
            cols = pl.ds(h * HEAD_DIM, HEAD_DIM)
            qb, kb, vb, dob = q[rows, cols], k[rows, cols], v[rows, cols], do[rows, cols]
            a, b = a_s[block, h], b_s[block, h]
            s = (s_in[h] + kv_s[block, h]).astype(BF16)
            r = (r_in[h] + qdo_s[block, h]).astype(BF16)

            def both(left, right, top, bottom):
                out = dot(jnp.concatenate([left, right], axis=1), jnp.concatenate([top, bottom], axis=0))
                return (out * scale).astype(BF16)

            o[rows, cols] = both(a, qb, vb, s)
            dq[rows, cols] = both(b, dob, kb, s.T)
            k[rows, cols] = both(b.T, vb, qb, r.T)
            v[rows, cols] = both(a.T, kb, dob, r)

    outs = [pltpu.make_async_copy(o, xo_out.at[:, pl.ds(dim, width)], out_sems.at[2])]
    for index, (src, column) in enumerate(((dq, 0), (k, width + dim), (v, 2 * width + dim))):
        outs.append(pltpu.make_async_copy(src, ra_out.at[:, pl.ds(column, width)], out_sems.at[3 + index]))
    for copy in outs:
        copy.start()
    for which, last in ((0, n_chips - 1), (1, 0)):
        @pl.when(chip != last)
        def _():
            for h in range(n_heads):
                chain_copy(which, h).wait_send()
    for copy in outs + [x_out, dy_out]:
        copy.wait()


def ring(n_seq):
    core, chip, n_chips, peer = position(n_seq)
    me = lax.axis_index("sp")
    rank = (1 - core) * chip + core * lax.rem(n_chips - chip, n_chips)
    following = lax.rem(me + 2 - 4 * core + n_seq, n_seq)
    previous = lax.rem(me - 2 + 4 * core + n_seq, n_seq)
    return core, rank, n_chips, peer, following, previous


def tile_slot(chunk, piece, early):
    return chunk * early + lax.rem(piece, early), lax.div(piece, early)


def reduce_kernel(n_seq, xo, ra, red_out, own_out, grads, red, send_sems, recv_sems, own_sems, out_sem):
    core, rank, n_chips, peer, following, previous = ring(n_seq)
    n_slots, _, width = grads.shape
    dim = 2 * width
    per_weight = dim // TILE
    early = 2 * per_weight // n_chips
    pieces = 2 * early
    n_rows = own_out.shape[1]

    entry_barrier((peer, following, previous))
    own_rows, peer_rows = aligned(core, n_rows), aligned(1 - core, n_rows)
    cols = aligned(core, width)
    copies = []
    for index, (src, column) in enumerate(((xo, dim), (ra, 0), (ra, width + dim), (ra, 2 * width + dim))):
        part = pl.ds(column, width)
        copies.append(pltpu.make_async_copy(src.at[own_rows, part], own_out.at[index, :, cols], own_sems.at[index, 0]))
        copies.append(send(src.at[peer_rows, part], own_out.at[index, :, cols], own_sems.at[index, 1], own_sems.at[index, 2], peer))

    def term(chunk, piece):
        unit, late = tile_slot(chunk, piece, early)
        inside = lax.rem(unit, per_weight)
        second = lax.div(unit, per_weight)
        is_o = (1 - late) * second
        left = (1 - is_o) * inside + is_o * (per_weight + lax.div(inside, 2))
        right = (1 - late) * is_o * (1 + lax.rem(inside, 2)) + late * (3 + second)
        return dot_t(xo[:, aligned(left, TILE)], ra[:, aligned(right, width)])

    def slot_of(chunk, piece):
        unit, late = tile_slot(chunk, piece, early)
        return unit + late * (n_slots // 2)

    def hop(step, piece):
        slot = slot_of(lax.rem(rank - step + n_chips, n_chips), piece)
        return send(grads.at[slot], grads.at[slot], send_sems.at[step, piece], recv_sems.at[step, piece], following)

    def arrival(step, piece):
        slot = slot_of(lax.rem(rank - step - 1 + n_chips, n_chips), piece)
        return send(grads.at[slot], grads.at[slot], send_sems.at[step, piece], recv_sems.at[step, piece], following)

    @pl.loop(0, pieces)
    def _(piece):
        grads[slot_of(rank, piece)] = term(rank, piece)
        hop(0, piece).start()

    for copy in copies:
        copy.start()

    @pl.loop(1, n_chips)
    def _(step):
        @pl.loop(0, pieces)
        def _(piece):
            chunk = lax.rem(rank - step + n_chips, n_chips)
            slot = slot_of(chunk, piece)
            mine = term(chunk, piece)
            arrival(step - 1, piece).wait_recv()

            @pl.when(step < n_chips - 1)
            def _():
                grads[slot] = grads[slot] + mine
                hop(step, piece).start()

            @pl.when(step == n_chips - 1)
            def _():
                red[piece] = grads[slot] + mine

    result = pltpu.make_async_copy(red, red_out, out_sem)
    result.start()

    @pl.loop(0, n_chips - 1)
    def _(step):
        @pl.loop(0, pieces)
        def _(piece):
            hop(step, piece).wait_send()

    for copy in copies:
        copy.wait()
    result.wait()


def gather_kernel(n_seq, red, own, wq, wk, wv, wo, both_out, y_out, dx_out, own_s, wo_s, w_s, y_s, dx_s, own_sems, w_sems, res_sems, send_sems, recv_sems, peer_sems):
    core, rank, n_chips, peer, following, previous = ring(n_seq)
    mine_out, peer_out = both_out.at[0], both_out.at[1]
    n_slots, _, width = mine_out.shape
    dim = 2 * width
    early = 2 * (dim // TILE) // n_chips
    pieces = 2 * early
    n_rows = own.shape[1]
    unit_cols = wo_s.shape[2]
    n_units = dim // unit_cols
    row_blocks = n_rows // ROWS

    def slot_of(chunk, piece):
        unit, late = tile_slot(chunk, piece, early)
        return unit + late * (n_slots // 2)

    def held(step, piece):
        return slot_of(lax.rem(rank + 1 - step + n_chips, n_chips), piece)

    def w_loads(unit, buffer):
        part = aligned(unit, unit_cols)
        loads = [pltpu.make_async_copy(wo.at[:, part], wo_s.at[buffer], w_sems.at[buffer, 0])]
        for index, weight in enumerate((wq, wk, wv)):
            loads.append(pltpu.make_async_copy(weight.at[part], w_s.at[buffer, index], w_sems.at[buffer, 1 + index]))
        return loads

    def results(unit, buffer):
        part = aligned(unit, unit_cols)
        return [pltpu.make_async_copy(src.at[buffer], dst.at[:, part], res_sems.at[buffer, index]) for index, (src, dst) in enumerate(((y_s, y_out), (dx_s, dx_out)))]

    own_load = pltpu.make_async_copy(own, own_s, own_sems.at[0])
    own_load.start()
    for unit in range(2):
        for load in w_loads(unit, unit):
            load.start()
    red_loads = [pltpu.make_async_copy(red.at[piece], mine_out.at[held(0, piece)], own_sems.at[1 + piece]) for piece in range(pieces)]
    for load in red_loads:
        load.start()

    entry_barrier((peer, following, previous))

    def to_next(step, piece):
        slot = held(step, piece)
        return send(mine_out.at[slot], mine_out.at[slot], send_sems.at[step, piece], recv_sems.at[step, piece], following)

    def arrival(step, piece):
        slot = held(step + 1, piece)
        return send(mine_out.at[slot], mine_out.at[slot], send_sems.at[step, piece], recv_sems.at[step, piece], following)

    def to_peer(step, piece):
        slot = held(step, piece)
        return send(mine_out.at[slot], peer_out.at[slot], peer_sems.at[0, step, piece], peer_sems.at[1, step, piece], peer)

    for piece in range(pieces):
        red_loads[piece].wait()
        to_next(0, piece).start()
        to_peer(0, piece).start()
    own_load.wait()

    def project(unit, block):
        buffer = lax.rem(unit, 2)

        @pl.when(block == 0)
        def _():
            for load in w_loads(unit, buffer):
                load.wait()

            @pl.when(unit >= 2)
            def _():
                for copy in results(unit - 2, buffer):
                    copy.wait()

        rows = aligned(block, ROWS)
        y_s[buffer, rows, :] = dot(own_s[0, rows, :], wo_s[buffer]).astype(BF16)
        total = dot_nt(own_s[1, rows, :], w_s[buffer, 0])
        total += dot_nt(own_s[2, rows, :], w_s[buffer, 1])
        total += dot_nt(own_s[3, rows, :], w_s[buffer, 2])
        dx_s[buffer, rows, :] = total.astype(BF16)

        @pl.when(block == row_blocks - 1)
        def _():
            for copy in results(unit, buffer):
                copy.start()

            @pl.when(unit + 2 < n_units)
            def _():
                for load in w_loads(unit + 2, buffer):
                    load.start()

    @pl.loop(0, (n_chips - 1) * pieces)
    def _(index):
        step, piece = lax.div(index, pieces), lax.rem(index, pieces)

        @pl.when(index < n_units * row_blocks)
        def _():
            project(lax.div(index, row_blocks), lax.rem(index, row_blocks))

        arrival(step, piece).wait_recv()

        @pl.when(step < n_chips - 2)
        def _():
            to_next(step + 1, piece).start()

        to_peer(step + 1, piece).start()

    @pl.loop(0, n_chips * pieces)
    def _(index):
        step, piece = lax.div(index, pieces), lax.rem(index, pieces)

        @pl.when(step < n_chips - 1)
        def _():
            to_next(step, piece).wait_send()

        to_peer(step, piece).wait()

    for unit in range(n_units - 2, n_units):
        for copy in results(unit, unit % 2):
            copy.wait()


def place_kernel(both, gq, gk, gv, go, sems):
    core = lax.rem(lax.axis_index("sp"), 2)
    _, n_slots, _, width = both.shape
    per_weight = n_slots // 4
    copies = []
    for side, half in enumerate((core, 1 - core)):
        cols = aligned(half, width)
        for slot in range(n_slots):
            weight, inside = slot // per_weight, slot % per_weight
            if weight == 1:
                rows = pl.ds(pl.multiple_of(half * width + inside // 2 * TILE, TILE), TILE)
                dst = go.at[rows, pl.ds(inside % 2 * width, width)]
            else:
                dst = (gq, None, gk, gv)[weight].at[pl.ds(inside * TILE, TILE), cols]
            copies.append(pltpu.make_async_copy(both.at[side, slot], dst, sems.at[side]))
    for copy in copies:
        copy.start()
    for copy in copies:
        copy.wait()


def solution(mesh):
    n_seq = mesh.shape["sp"]
    n_chips = n_seq // 2
    row_spec = P(("dp", "sp"), None)
    grad_spec = P("dp", None)
    any_spec = pl.BlockSpec(memory_space=pl.ANY)
    vmem_spec = pl.BlockSpec(memory_space=pltpu.VMEM)
    dma = pltpu.SemaphoreType.DMA

    def params(collective_id, limit=VMEM_LIMIT):
        return pltpu.CompilerParams(collective_id=collective_id, has_side_effects=True, vmem_limit_bytes=limit)

    def local_layer(tokens, w_q, w_k, w_v, w_o, grad_y):
        n_rows, dim = tokens.shape
        width = dim // 2
        n_heads = width // HEAD_DIM
        rows = 2 * n_rows
        n_blocks = rows // BLOCK_LEN
        n_slots = 4 * (dim // TILE)
        pieces = n_slots // n_chips
        scale = 1.0 / math.sqrt(n_rows * n_seq * HEAD_DIM)
        state = (n_heads, HEAD_DIM, HEAD_DIM)

        xo, ra = pl.pallas_call(
            functools.partial(attention_kernel, n_seq, scale),
            out_shape=(jax.ShapeDtypeStruct((rows, dim + width), BF16), jax.ShapeDtypeStruct((rows, dim + 3 * width), BF16)),
            in_specs=[any_spec] * 6,
            out_specs=(any_spec,) * 2,
            scratch_shapes=[pltpu.VMEM((rows, dim), BF16)] * 2
            + [pltpu.VMEM((3, dim, width), BF16), pltpu.VMEM((width, dim), BF16)]
            + [pltpu.VMEM((rows, width), BF16)] * 6
            + [pltpu.VMEM((n_blocks, n_heads, BLOCK_LEN, BLOCK_LEN), BF16)] * 2
            + [pltpu.VMEM((n_blocks,) + state, F32)] * 2
            + [pltpu.VMEM(state, F32)] * 4
            + [dma((2, 3)), dma((4,)), dma((2, 2, n_heads)), dma((6,))],
            compiler_params=params(0),
            name="attention",
        )(tokens, grad_y, w_q, w_k, w_v, w_o)

        red, own = pl.pallas_call(
            functools.partial(reduce_kernel, n_seq),
            out_shape=(jax.ShapeDtypeStruct((pieces, TILE, width), F32), jax.ShapeDtypeStruct((4, n_rows, dim), BF16)),
            in_specs=[vmem_spec] * 2,
            out_specs=(any_spec,) * 2,
            scratch_shapes=[pltpu.VMEM((n_slots, TILE, width), F32), pltpu.VMEM((pieces, TILE, width), F32)]
            + [dma((n_chips - 1, pieces))] * 2 + [dma((4, 3)), dma],
            compiler_params=params(1),
            name="reduce",
        )(xo, ra)

        unit_cols = min(256, dim // 2)
        halves = (2, n_slots, TILE, width)
        both, out_y, grad_x = pl.pallas_call(
            functools.partial(gather_kernel, n_seq),
            out_shape=(pltpu.VMEM(halves, F32), jax.ShapeDtypeStruct((n_rows, dim), BF16), jax.ShapeDtypeStruct((n_rows, dim), BF16)),
            in_specs=[any_spec] * 6,
            out_specs=(vmem_spec, any_spec, any_spec),
            scratch_shapes=[pltpu.VMEM((4, n_rows, dim), BF16), pltpu.VMEM((2, dim, unit_cols), BF16), pltpu.VMEM((2, 3, unit_cols, dim), BF16)]
            + [pltpu.VMEM((2, n_rows, unit_cols), BF16)] * 2
            + [dma((1 + pieces,)), dma((2, 4)), dma((2, 2)), dma((n_chips - 1, pieces)), dma((n_chips - 1, pieces)), dma((2, n_chips, pieces))],
            compiler_params=params(2, VMEM_LIMIT - math.prod(halves) * 4 - (1 << 20)),
            name="gather",
        )(red, own, w_q, w_k, w_v, w_o)

        grads = pl.pallas_call(
            place_kernel,
            out_shape=(jax.ShapeDtypeStruct((dim, dim), F32),) * 4,
            in_specs=[vmem_spec],
            out_specs=(any_spec,) * 4,
            scratch_shapes=[dma((2,))],
            compiler_params=pltpu.CompilerParams(vmem_limit_bytes=1 << 20),
            name="place",
        )(both)
        return (out_y, grad_x) + tuple(grads)

    return jax.shard_map(local_layer, mesh=mesh, in_specs=(row_spec, P(), P(), P(), P(), row_spec), out_specs=(row_spec, row_spec, grad_spec, grad_spec, grad_spec, grad_spec), check_vma=False)
```

```python
import functools
import math
import jax
import jax.numpy as jnp
from jax import lax
from jax.experimental import pallas as pl
from jax.experimental.pallas import tpu as pltpu
from jax.sharding import PartitionSpec as P

HEAD_DIM = 128
BLOCK_LEN = 128
TILE = 128
ROWS = 256
MESH = pl.DeviceIdType.MESH
VMEM_LIMIT = 67_043_328
F32 = jnp.float32
BF16 = jnp.bfloat16


def dot_t(lhs, rhs):
    return lax.dot_general(lhs, rhs, (((0,), (0,)), ((), ())), preferred_element_type=F32)


def dot_nt(lhs, rhs):
    return lax.dot_general(lhs, rhs, (((1,), (1,)), ((), ())), preferred_element_type=F32)


def dot(lhs, rhs):
    return jnp.dot(lhs, rhs, preferred_element_type=F32)


def aligned(index, size):
    return pl.ds(pl.multiple_of(index * size, size), size)


def position(n_seq):
    me = lax.axis_index("sp")
    core, chip = lax.rem(me, 2), lax.div(me, 2)
    return core, chip, n_seq // 2, me + 1 - 2 * core


def send(src, dst, send_sem, recv_sem, target):
    return pltpu.make_async_remote_copy(src_ref=src, dst_ref=dst, send_sem=send_sem, recv_sem=recv_sem, device_id={"sp": target}, device_id_type=MESH)


def entry_barrier(targets):
    barrier = pltpu.get_barrier_semaphore()
    for target in targets:
        pl.semaphore_signal(barrier, inc=1, device_id={"sp": target}, device_id_type=MESH)
    pl.semaphore_wait(barrier, len(targets))


def ring(n_seq):
    core, chip, n_chips, peer = position(n_seq)
    me = lax.axis_index("sp")
    rank = (1 - core) * chip + core * lax.rem(n_chips - chip, n_chips)
    following = lax.rem(me + 2 - 4 * core + n_seq, n_seq)
    previous = lax.rem(me - 2 + 4 * core + n_seq, n_seq)
    return core, rank, n_chips, peer, following, previous


def attention_kernel(n_seq, scale, x, dy, wq, wk, wv, wo, red_out, own_out, xo, ra, w_s, q, do, grads, land, s_in, s_out, r_in, r_out, x_sems, w_sems, chain_sems, send_sems, recv_sems, own_sems, red_sems, credits):
    _, chip, _, _ = position(n_seq)
    core, rank, n_chips, peer, following, previous = ring(n_seq)
    me = lax.axis_index("sp")
    up, down = lax.rem(me + 2, n_seq), lax.rem(me + n_seq - 2, n_seq)
    n_rows, dim = x.shape
    all_rows, width = q.shape
    n_heads = width // HEAD_DIM
    n_blocks = all_rows // BLOCK_LEN
    n_slots = grads.shape[0]
    per_weight = dim // TILE
    early = 2 * per_weight // n_chips
    own_rows, peer_rows = aligned(core, n_rows), aligned(1 - core, n_rows)
    w_cols = aligned(core, width)
    k_col, v_col, a_row, b_row = width + dim, 2 * width + dim, 0, all_rows
    kv_slot, qdo_slot = 0, n_slots // 2

    entry_barrier((peer, up, down))
    x_part, dy_part = pl.ds(0, dim), pl.ds(width, dim)
    local, remote = [], []
    for index, (src, dst) in enumerate(((x, xo.at[own_rows, x_part]), (dy, ra.at[own_rows, dy_part]))):
        remote.append(send(src, dst, x_sems.at[index, 0], x_sems.at[index, 1], peer))
        local.append(pltpu.make_async_copy(src, dst, x_sems.at[index, 2]))
    w_loads = [pltpu.make_async_copy(weight.at[:, w_cols], w_s.at[pl.ds(index * dim, dim)], w_sems.at[index]) for index, weight in enumerate((wk, wv, wq))]
    for part in range(2):
        w_loads.append(pltpu.make_async_copy(wo.at[w_cols, pl.ds(part * width, width)], w_s.at[pl.ds(3 * dim + part * width, width)], w_sems.at[3 + part]))
    remote[0].start()
    local[0].start()
    for load in w_loads[:2]:
        load.start()
    remote[1].start()
    for load in w_loads[2:]:
        load.start()
    local[1].start()

    def weight(index, size):
        return w_s[pl.ds(index * size, size), :]

    def part_rows(half, step):
        return pl.ds(pl.multiple_of(half * n_rows + step * ROWS, ROWS), ROWS)

    def project_kv(half):
        @pl.loop(0, n_rows // ROWS)
        def _(step):
            rows = part_rows(half, step)
            ra[rows, pl.ds(k_col, width)] = dot(xo[rows, x_part], weight(0, dim)).astype(BF16)
            ra[rows, pl.ds(v_col, width)] = dot(xo[rows, x_part], weight(1, dim)).astype(BF16)

    local[0].wait()
    w_loads[0].wait()
    w_loads[1].wait()
    project_kv(core)
    remote[0].wait()
    project_kv(1 - core)

    def head(h, column=0):
        return pl.ds(column + h * HEAD_DIM, HEAD_DIM)

    def accumulate(left, right, slot, total, reverse):
        total[...] = jnp.zeros_like(total)

        @pl.loop(0, n_blocks)
        def _(step):
            block = (n_blocks - 1 - step) if reverse else step
            rows = aligned(block, BLOCK_LEN)
            for h in range(n_heads):
                running = total[h]
                grads[slot + block, :, head(h)] = running
                total[h] = running + dot_t(left(rows, h), right(rows, h))

    def q_of(rows, h):
        return q[rows, head(h)]

    def do_of(rows, h):
        return do[rows, head(h)]

    def k_of(rows, h):
        return ra[rows, head(h, k_col)]

    def v_of(rows, h):
        return ra[rows, head(h, v_col)]

    def chain_copy(which, h):
        src, dst, target = ((s_out, s_in, up), (r_out, r_in, down))[which]
        return send(src.at[h], dst.at[h], chain_sems.at[which, 0, h], chain_sems.at[which, 1, h], target)

    def chain_step(which, h):
        first, last = ((0, n_chips - 1), (n_chips - 1, 0))[which]
        src, dst = ((s_out, s_in), (r_out, r_in))[which]

        @pl.when(chip == first)
        def _():
            dst[h] = jnp.zeros_like(dst[h])

        @pl.when(chip != first)
        def _():
            chain_copy(which, h).wait_recv()
            src[h] = src[h] + dst[h]

        @pl.when(chip != last)
        def _():
            chain_copy(which, h).start()

    def chain_s(tick):
        @pl.when((tick >= 3 * chip) & (tick < 3 * chip + n_heads))
        def _():
            chain_step(0, tick - 3 * chip)

    accumulate(k_of, v_of, kv_slot, s_out, False)

    steps = n_rows // ROWS

    def project_qdo(half, first_tick):
        @pl.loop(0, steps)
        def _(step):
            chain_s(first_tick + step)
            rows = part_rows(half, step)
            q[rows, :] = dot(xo[rows, x_part], weight(2, dim)).astype(BF16)
            product = dot_nt(ra[rows, pl.ds(width, width)], weight(6, width))
            product += dot_nt(ra[rows, pl.ds(2 * width, width)], weight(7, width))
            do[rows, :] = product.astype(BF16)

    for load in w_loads[2:] + [local[1]]:
        load.wait()
    project_qdo(core, 0)
    remote[1].wait()
    project_qdo(1 - core, steps)

    causal = lax.broadcasted_iota(jnp.int32, (BLOCK_LEN, BLOCK_LEN), 0) >= lax.broadcasted_iota(jnp.int32, (BLOCK_LEN, BLOCK_LEN), 1)

    def block_scores(block):
        rows = aligned(block, BLOCK_LEN)
        a_rows = pl.ds(pl.multiple_of(a_row + block * BLOCK_LEN, BLOCK_LEN), BLOCK_LEN)
        b_rows = pl.ds(pl.multiple_of(b_row + block * BLOCK_LEN, BLOCK_LEN), BLOCK_LEN)
        for h in range(n_heads):
            w_s[a_rows, head(h)] = jnp.where(causal, dot_nt(q_of(rows, h), k_of(rows, h)), 0.0).astype(BF16)
            w_s[b_rows, head(h)] = jnp.where(causal, dot_nt(do_of(rows, h), v_of(rows, h)), 0.0).astype(BF16)

    @pl.loop(0, max(3 * (n_chips - 1) + n_heads - 2 * steps, n_blocks))
    def _(step):
        chain_s(2 * steps + step)

        @pl.when(step < n_blocks)
        def _():
            block_scores(step)

    def scores(block, h):
        a_rows = pl.ds(pl.multiple_of(a_row + block * BLOCK_LEN, BLOCK_LEN), BLOCK_LEN)
        b_rows = pl.ds(pl.multiple_of(b_row + block * BLOCK_LEN, BLOCK_LEN), BLOCK_LEN)
        return w_s[a_rows, head(h)], w_s[b_rows, head(h)]

    def both(left, right, top, bottom):
        out = dot(jnp.concatenate([left, right], axis=1), jnp.concatenate([top, bottom], axis=0))
        return (out * scale).astype(BF16)

    @pl.loop(0, n_blocks)
    def _(block):
        rows = aligned(block, BLOCK_LEN)
        for h in range(n_heads):
            a, b = scores(block, h)
            s = (s_in[h] + grads[kv_slot + block, :, head(h)]).astype(BF16)
            xo[rows, head(h, dim)] = both(a, q_of(rows, h), v_of(rows, h), s)
            ra[rows, head(h)] = both(b, do_of(rows, h), k_of(rows, h), s.T)

    def rev_block(block):
        rows = aligned(block, BLOCK_LEN)
        for h in range(n_heads):
            a, b = scores(block, h)
            r = (r_in[h] + grads[qdo_slot + block, :, head(h)]).astype(BF16)
            dk = both(b.T, v_of(rows, h), q_of(rows, h), r.T)
            dv = both(a.T, k_of(rows, h), do_of(rows, h), r)
            ra[rows, head(h, k_col)] = dk
            ra[rows, head(h, v_col)] = dv

    def credit(which):
        pl.semaphore_signal(credits.at[which], inc=1, device_id={"sp": previous}, device_id_type=MESH)

    def term(late, unit):
        inside, second = lax.rem(unit, per_weight), lax.div(unit, per_weight)
        if late:
            left, right = inside, 3 + second
        else:
            left = (1 - second) * inside + second * (per_weight + lax.div(inside, 2))
            right = second * (1 + lax.rem(inside, 2))
        return dot_t(xo[:, aligned(left, TILE)], ra[:, aligned(right, width)])

    def unit_of(step, piece):
        return lax.rem(rank - step + n_chips, n_chips) * early + piece

    def hop(late, step, piece):
        slot = grads.at[late * (n_slots // 2) + unit_of(step, piece)]
        sems = send_sems.at[late, step, piece], recv_sems.at[late, step, piece]
        return slot, sems

    def start_hop(late, step, piece, first):
        slot, sems = hop(late, step, piece)
        send(slot, land.at[late * early + piece] if first else slot, *sems, following).start()

    def run_ring(late, extra):
        offset = late * (n_slots // 2)

        @pl.loop(0, early)
        def _(piece):
            unit = unit_of(0, piece)
            grads[offset + unit] = term(late, unit)
            start_hop(late, 0, piece, True)

        @pl.loop(0, (n_chips - 1) * early)
        def _(index):
            step, piece = lax.div(index, early) + 1, lax.rem(index, early)
            unit = unit_of(step, piece)
            slot = offset + unit
            extra(index)
            mine = term(late, unit)

            @pl.when(step == 1)
            def _():
                place = land.at[late * early + piece]
                send(place, place, send_sems.at[late, 0, piece], recv_sems.at[late, 0, piece], following).wait_recv()
                grads[slot] = place[...] + mine

            @pl.when(step > 1)
            def _():
                place = grads.at[slot]
                send(place, place, send_sems.at[late, step - 1, piece], recv_sems.at[late, step - 1, piece], following).wait_recv()
                grads[slot] = grads[slot] + mine

            @pl.when(index == 0)
            def _():
                pl.semaphore_wait(credits.at[late], 1)

            @pl.when(step < n_chips - 1)
            def _():
                start_hop(late, step, piece, False)

            @pl.when(step == n_chips - 1)
            def _():
                pltpu.make_async_copy(grads.at[slot], red_out.at[late * early + piece], red_sems.at[late * early + piece]).start()

    share = n_blocks // 4

    def reverse_work(index):
        @pl.when(index == 0)
        def _():
            accumulate(q_of, do_of, qdo_slot, r_out, True)

        @pl.when(index == n_chips - chip)
        def _():
            for h in range(n_heads):
                chain_step(1, h)

        @pl.when((index > n_chips) & (index <= n_chips + 4))
        def _():
            @pl.loop(0, share)
            def _(part):
                rev_block((index - n_chips - 1) * share + part)

        @pl.when(index == n_chips + 4)
        def _():
            credit(1)

    credit(0)
    run_ring(0, reverse_work)

    copies = []
    for index, (src, column) in enumerate(((xo, dim), (ra, 0), (ra, k_col), (ra, v_col))):
        part = pl.ds(column, width)
        copies.append(pltpu.make_async_copy(src.at[own_rows, part], own_out.at[index, :, w_cols], own_sems.at[index, 0]))
        copies.append(send(src.at[peer_rows, part], own_out.at[index, :, w_cols], own_sems.at[index, 1], own_sems.at[index, 2], peer))
    for copy in copies:
        copy.start()

    run_ring(1, lambda index: None)

    for which, last in ((0, n_chips - 1), (1, 0)):
        @pl.when(chip != last)
        def _():
            for h in range(n_heads):
                chain_copy(which, h).wait_send()

    for late in range(2):
        @pl.loop(0, (n_chips - 1) * early)
        def _(index):
            step, piece = lax.div(index, early), lax.rem(index, early)
            slot, sems = hop(late, step, piece)
            send(slot, slot, *sems, following).wait_send()

    for copy in copies:
        copy.wait()
    for late in range(2):
        for piece in range(early):
            slot = late * (n_slots // 2) + lax.rem(rank + 1, n_chips) * early + piece
            pltpu.make_async_copy(grads.at[slot], red_out.at[late * early + piece], red_sems.at[late * early + piece]).wait()


def tile_slot(chunk, piece, early):
    return chunk * early + lax.rem(piece, early), lax.div(piece, early)


def gather_kernel(n_seq, red, own, wq, wk, wv, wo, rows_out, both_out, own_s, wo_s, w_s, own_sems, w_sems, send_sems, recv_sems, peer_sems):
    core, rank, n_chips, peer, following, previous = ring(n_seq)
    mine_out, peer_out = both_out.at[0], both_out.at[1]
    y_out, dx_out = rows_out.at[0], rows_out.at[1]
    n_slots, _, width = mine_out.shape
    dim = 2 * width
    early = 2 * (dim // TILE) // n_chips
    pieces = 2 * early
    n_rows = own.shape[1]
    unit_cols = wo_s.shape[2]
    n_units = dim // unit_cols
    row_blocks = n_rows // ROWS

    def slot_of(chunk, piece):
        unit, late = tile_slot(chunk, piece, early)
        return unit + late * (n_slots // 2)

    def held(step, piece):
        return slot_of(lax.rem(rank + 1 - step + n_chips, n_chips), piece)

    def w_loads(unit, buffer):
        part = aligned(unit, unit_cols)
        loads = [pltpu.make_async_copy(wo.at[:, part], wo_s.at[buffer], w_sems.at[buffer, 0])]
        for index, weight in enumerate((wq, wk, wv)):
            loads.append(pltpu.make_async_copy(weight.at[part], w_s.at[buffer, index], w_sems.at[buffer, 1 + index]))
        return loads

    own_load = pltpu.make_async_copy(own, own_s, own_sems.at[0])
    own_load.start()
    for unit in range(2):
        for load in w_loads(unit, unit):
            load.start()
    red_loads = [pltpu.make_async_copy(red.at[piece], mine_out.at[held(0, piece)], own_sems.at[1 + piece]) for piece in range(pieces)]
    for load in red_loads:
        load.start()

    entry_barrier((peer, following, previous))

    def to_next(step, piece):
        slot = held(step, piece)
        return send(mine_out.at[slot], mine_out.at[slot], send_sems.at[step, piece], recv_sems.at[step, piece], following)

    def arrival(step, piece):
        slot = held(step + 1, piece)
        return send(mine_out.at[slot], mine_out.at[slot], send_sems.at[step, piece], recv_sems.at[step, piece], following)

    def to_peer(step, piece):
        slot = held(step, piece)
        return send(mine_out.at[slot], peer_out.at[slot], peer_sems.at[0, step, piece], peer_sems.at[1, step, piece], peer)

    for piece in range(pieces):
        red_loads[piece].wait()
        to_next(0, piece).start()
        to_peer(0, piece).start()
    own_load.wait()

    def project(unit, block):
        buffer = lax.rem(unit, 2)

        @pl.when(block == 0)
        def _():
            for load in w_loads(unit, buffer):
                load.wait()

        rows, cols = aligned(block, ROWS), aligned(unit, unit_cols)
        y_out[rows, cols] = dot(own_s[0, rows, :], wo_s[buffer]).astype(BF16)
        total = dot_nt(own_s[1, rows, :], w_s[buffer, 0])
        total += dot_nt(own_s[2, rows, :], w_s[buffer, 1])
        total += dot_nt(own_s[3, rows, :], w_s[buffer, 2])
        dx_out[rows, cols] = total.astype(BF16)

        @pl.when((block == row_blocks - 1) & (unit + 2 < n_units))
        def _():
            for load in w_loads(unit + 2, buffer):
                load.start()

    @pl.loop(0, (n_chips - 1) * pieces)
    def _(index):
        step, piece = lax.div(index, pieces), lax.rem(index, pieces)

        @pl.when(index < n_units * row_blocks)
        def _():
            project(lax.div(index, row_blocks), lax.rem(index, row_blocks))

        arrival(step, piece).wait_recv()

        @pl.when(step < n_chips - 2)
        def _():
            to_next(step + 1, piece).start()

        to_peer(step + 1, piece).start()

    @pl.loop(0, n_chips * pieces)
    def _(index):
        step, piece = lax.div(index, pieces), lax.rem(index, pieces)

        @pl.when(step < n_chips - 1)
        def _():
            to_next(step, piece).wait_send()

        to_peer(step, piece).wait()


def place_kernel(results, both, y, dx, gq, gk, gv, go, sems):
    core = lax.rem(lax.axis_index("sp"), 2)
    _, n_slots, _, width = both.shape
    per_weight = n_slots // 4
    copies = [pltpu.make_async_copy(results.at[0], y, sems.at[2]), pltpu.make_async_copy(results.at[1], dx, sems.at[3])]
    for side, half in enumerate((core, 1 - core)):
        cols = aligned(half, width)
        for slot in range(n_slots):
            weight, inside = slot // per_weight, slot % per_weight
            if weight == 1:
                rows = pl.ds(pl.multiple_of(half * width + inside // 2 * TILE, TILE), TILE)
                dst = go.at[rows, pl.ds(inside % 2 * width, width)]
            else:
                dst = (gq, None, gk, gv)[weight].at[pl.ds(inside * TILE, TILE), cols]
            copies.append(pltpu.make_async_copy(both.at[side, slot], dst, sems.at[side]))
    for copy in copies:
        copy.start()
    for copy in copies:
        copy.wait()


def solution(mesh):
    n_seq = mesh.shape["sp"]
    n_chips = n_seq // 2
    row_spec = P(("dp", "sp"), None)
    grad_spec = P("dp", None)
    any_spec = pl.BlockSpec(memory_space=pl.ANY)
    vmem_spec = pl.BlockSpec(memory_space=pltpu.VMEM)
    dma = pltpu.SemaphoreType.DMA

    def params(collective_id, limit=VMEM_LIMIT):
        return pltpu.CompilerParams(collective_id=collective_id, has_side_effects=True, vmem_limit_bytes=limit)

    def local_layer(tokens, w_q, w_k, w_v, w_o, grad_y):
        n_rows, dim = tokens.shape
        width = dim // 2
        n_heads = width // HEAD_DIM
        rows = 2 * n_rows
        n_slots = 4 * (dim // TILE)
        pieces = n_slots // n_chips
        scale = 1.0 / math.sqrt(n_rows * n_seq * HEAD_DIM)
        state = (n_heads, HEAD_DIM, HEAD_DIM)

        red, own = pl.pallas_call(
            functools.partial(attention_kernel, n_seq, scale),
            out_shape=(jax.ShapeDtypeStruct((pieces, TILE, width), F32), jax.ShapeDtypeStruct((4, n_rows, dim), BF16)),
            in_specs=[any_spec] * 6,
            out_specs=(any_spec,) * 2,
            scratch_shapes=[pltpu.VMEM((rows, dim + width), BF16), pltpu.VMEM((rows, dim + 3 * width), BF16), pltpu.VMEM((4 * dim, width), BF16)]
            + [pltpu.VMEM((rows, width), BF16)] * 2
            + [pltpu.VMEM((n_slots, TILE, width), F32), pltpu.VMEM((pieces, TILE, width), F32)]
            + [pltpu.VMEM(state, F32)] * 4
            + [dma((2, 3)), dma((5,)), dma((2, 2, n_heads))]
            + [dma((2, n_chips - 1, pieces // 2))] * 2
            + [dma((4, 3)), dma((pieces,)), pltpu.SemaphoreType.REGULAR((2,))],
            compiler_params=params(0),
            name="attention",
        )(tokens, grad_y, w_q, w_k, w_v, w_o)

        unit_cols = min(256, dim // 2)
        halves = (2, n_slots, TILE, width)
        room = VMEM_LIMIT - math.prod(halves) * 4 - 4 * n_rows * dim - (1 << 20)
        results = pl.pallas_call(
            functools.partial(gather_kernel, n_seq),
            out_shape=(pltpu.VMEM((2, n_rows, dim), BF16), pltpu.VMEM(halves, F32)),
            in_specs=[any_spec] * 6,
            out_specs=(vmem_spec,) * 2,
            scratch_shapes=[pltpu.VMEM((4, n_rows, dim), BF16), pltpu.VMEM((2, dim, unit_cols), BF16), pltpu.VMEM((2, 3, unit_cols, dim), BF16)]
            + [dma((1 + pieces,)), dma((2, 4)), dma((n_chips - 1, pieces)), dma((n_chips - 1, pieces)), dma((2, n_chips, pieces))],
            compiler_params=params(1, room),
            name="gather",
        )(red, own, w_q, w_k, w_v, w_o)

        return pl.pallas_call(
            place_kernel,
            out_shape=(jax.ShapeDtypeStruct((n_rows, dim), BF16),) * 2 + (jax.ShapeDtypeStruct((dim, dim), F32),) * 4,
            in_specs=[vmem_spec] * 2,
            out_specs=(any_spec,) * 6,
            scratch_shapes=[dma((4,))],
            compiler_params=pltpu.CompilerParams(vmem_limit_bytes=1 << 20),
            name="place",
        )(*results)

    return jax.shard_map(local_layer, mesh=mesh, in_specs=(row_spec, P(), P(), P(), P(), row_spec), out_specs=(row_spec, row_spec, grad_spec, grad_spec, grad_spec, grad_spec), check_vma=False)
```

```python
import functools
import math
import jax
import jax.numpy as jnp
from jax import lax
from jax.experimental import pallas as pl
from jax.experimental.pallas import tpu as pltpu
from jax.sharding import PartitionSpec as P

HEAD_DIM = 128
BLOCK_LEN = 128
TILE = 128
ROWS = 256
MESH = pl.DeviceIdType.MESH
VMEM_LIMIT = 67_043_328
F32 = jnp.float32
BF16 = jnp.bfloat16


def dot_t(lhs, rhs):
    return lax.dot_general(lhs, rhs, (((0,), (0,)), ((), ())), preferred_element_type=F32)


def dot_nt(lhs, rhs):
    return lax.dot_general(lhs, rhs, (((1,), (1,)), ((), ())), preferred_element_type=F32)


def dot(lhs, rhs):
    return jnp.dot(lhs, rhs, preferred_element_type=F32)


def aligned(index, size):
    return pl.ds(pl.multiple_of(index * size, size), size)


def position(n_seq):
    me = lax.axis_index("sp")
    core, chip = lax.rem(me, 2), lax.div(me, 2)
    return core, chip, n_seq // 2, me + 1 - 2 * core


def send(src, dst, send_sem, recv_sem, target):
    return pltpu.make_async_remote_copy(src_ref=src, dst_ref=dst, send_sem=send_sem, recv_sem=recv_sem, device_id={"sp": target}, device_id_type=MESH)


def entry_barrier(targets):
    barrier = pltpu.get_barrier_semaphore()
    for target in targets:
        pl.semaphore_signal(barrier, inc=1, device_id={"sp": target}, device_id_type=MESH)
    pl.semaphore_wait(barrier, len(targets))


def ring(n_seq):
    core, chip, n_chips, peer = position(n_seq)
    me = lax.axis_index("sp")
    rank = (1 - core) * chip + core * lax.rem(n_chips - chip, n_chips)
    following = lax.rem(me + 2 - 4 * core + n_seq, n_seq)
    previous = lax.rem(me - 2 + 4 * core + n_seq, n_seq)
    return core, rank, n_chips, peer, following, previous


def attention_kernel(n_seq, scale, x, dy, wq, wk, wv, wo, own_out, red_out, xo, ra, w_s, q, do, grads, land, s_in, s_out, s_even, s_pair, r_in, r_out, x_sems, w_sems, chain_sems, send_sems, recv_sems, own_sems, red_sems, credits):
    _, chip, _, _ = position(n_seq)
    core, rank, n_chips, peer, following, previous = ring(n_seq)
    me = lax.axis_index("sp")
    up, down = lax.rem(me + 2, n_seq), lax.rem(me + n_seq - 2, n_seq)
    up_two, down_two = lax.rem(me + 4, n_seq), lax.rem(me + n_seq - 4, n_seq)
    n_rows, dim = x.shape
    all_rows, width = q.shape
    n_heads = width // HEAD_DIM
    n_blocks = all_rows // BLOCK_LEN
    n_slots = grads.shape[0]
    per_weight = dim // TILE
    early = 2 * per_weight // n_chips
    own_rows, peer_rows = aligned(core, n_rows), aligned(1 - core, n_rows)
    w_cols = aligned(core, width)
    k_col, v_col, a_row, b_row = width + dim, 2 * width + dim, 0, all_rows
    kv_slot, qdo_slot = 0, n_slots // 2

    entry_barrier((peer, up, down, up_two, down_two))
    x_part, dy_part = pl.ds(0, dim), pl.ds(width, dim)
    local, remote = [], []
    for index, (src, dst) in enumerate(((x, xo.at[own_rows, x_part]), (dy, ra.at[own_rows, dy_part]))):
        remote.append(send(src, dst, x_sems.at[index, 0], x_sems.at[index, 1], peer))
        local.append(pltpu.make_async_copy(src, dst, x_sems.at[index, 2]))
    w_loads = [pltpu.make_async_copy(weight.at[:, w_cols], w_s.at[pl.ds(index * dim, dim)], w_sems.at[index]) for index, weight in enumerate((wk, wv, wq))]
    for part in range(2):
        w_loads.append(pltpu.make_async_copy(wo.at[w_cols, pl.ds(part * width, width)], w_s.at[pl.ds(3 * dim + part * width, width)], w_sems.at[3 + part]))
    remote[0].start()
    local[0].start()
    for load in w_loads[:2]:
        load.start()
    remote[1].start()
    for load in w_loads[2:]:
        load.start()
    local[1].start()

    def weight(index, size):
        return w_s[pl.ds(index * size, size), :]

    def part_rows(half, step):
        return pl.ds(pl.multiple_of(half * n_rows + step * ROWS, ROWS), ROWS)

    def project_kv(half):
        @pl.loop(0, n_rows // ROWS)
        def _(step):
            rows = part_rows(half, step)
            ra[rows, pl.ds(k_col, width)] = dot(xo[rows, x_part], weight(0, dim)).astype(BF16)
            ra[rows, pl.ds(v_col, width)] = dot(xo[rows, x_part], weight(1, dim)).astype(BF16)

    local[0].wait()
    w_loads[0].wait()
    w_loads[1].wait()
    project_kv(core)
    remote[0].wait()
    project_kv(1 - core)

    def head(h, column=0):
        return pl.ds(pl.multiple_of(column + h * HEAD_DIM, HEAD_DIM), HEAD_DIM)

    def accumulate(left, right, slot, total, reverse, extra):
        total[...] = jnp.zeros_like(total)

        @pl.loop(0, n_blocks)
        def _(step):
            block = (n_blocks - 1 - step) if reverse else step
            rows = aligned(block, BLOCK_LEN)
            extra(step)
            for h in range(n_heads):
                running = total[h]
                grads[slot + block, :, head(h)] = running
                total[h] = running + dot_t(left(rows, h), right(rows, h))

    def q_of(rows, h):
        return q[rows, head(h)]

    def do_of(rows, h):
        return do[rows, head(h)]

    def k_of(rows, h):
        return ra[rows, head(h, k_col)]

    def v_of(rows, h):
        return ra[rows, head(h, v_col)]

    odd = lax.rem(chip, 2)
    EVEN, PAIR, HAND, REV = range(4)

    def chain_copy(which, h):
        src, dst, target = ((s_out, s_even, up), (s_out, s_pair, up_two), (s_pair, s_in, down), (r_out, r_in, down))[which]
        return send(src.at[h], dst.at[h], chain_sems.at[which, 0, h], chain_sems.at[which, 1, h], target)

    def start_s():
        @pl.when(odd == 0)
        def _():
            for h in range(n_heads):
                chain_copy(EVEN, h).start()

    def odd_s(h):
        chain_copy(EVEN, h).wait_recv()

        @pl.when(chip == 1)
        def _():
            s_in[h] = s_even[h]

        @pl.when(chip != 1)
        def _():
            chain_copy(PAIR, h).wait_recv()
            chain_copy(HAND, h).start()
            s_in[h] = s_pair[h] + s_even[h]

        @pl.when(chip + 2 < n_chips)
        def _():
            s_out[h] = s_out[h] + s_in[h]
            chain_copy(PAIR, h).start()

    def even_s(h):
        @pl.when(chip == 0)
        def _():
            s_in[h] = jnp.zeros_like(s_in[h])

        @pl.when(chip != 0)
        def _():
            chain_copy(HAND, h).wait_recv()

    def chain_r(h):
        @pl.when(chip == n_chips - 1)
        def _():
            r_in[h] = jnp.zeros_like(r_in[h])

        @pl.when(chip != n_chips - 1)
        def _():
            chain_copy(REV, h).wait_recv()
            r_out[h] = r_out[h] + r_in[h]

        @pl.when(chip != 0)
        def _():
            chain_copy(REV, h).start()

    steps = n_rows // ROWS
    due = 3 + lax.div(7 * lax.div(chip, 2), 2)
    stride_r, stride_scores = n_blocks // 2, -(-n_blocks // 3)
    tick_r, tick_scores = 2 * steps, 2 * steps + 2
    last_tick = tick_scores + -(-n_blocks // stride_scores)

    def chain_s(tick):
        @pl.when((odd == 1) & (tick >= due) & (tick < due + n_heads))
        def _():
            odd_s(tick - due)

    accumulate(k_of, v_of, kv_slot, s_out, False, lambda step: None)
    start_s()

    def project_qdo(half, first_tick):
        @pl.loop(0, steps)
        def _(step):
            chain_s(first_tick + step)
            rows = part_rows(half, step)
            q[rows, :] = dot(xo[rows, x_part], weight(2, dim)).astype(BF16)
            product = dot_nt(ra[rows, pl.ds(width, width)], weight(6, width))
            product += dot_nt(ra[rows, pl.ds(2 * width, width)], weight(7, width))
            do[rows, :] = product.astype(BF16)

    for load in w_loads[2:] + [local[1]]:
        load.wait()
    project_qdo(core, 0)
    remote[1].wait()
    project_qdo(1 - core, steps)

    causal = lax.broadcasted_iota(jnp.int32, (BLOCK_LEN, BLOCK_LEN), 0) >= lax.broadcasted_iota(jnp.int32, (BLOCK_LEN, BLOCK_LEN), 1)

    def block_scores(block):
        rows = aligned(block, BLOCK_LEN)
        a_rows = pl.ds(pl.multiple_of(a_row + block * BLOCK_LEN, BLOCK_LEN), BLOCK_LEN)
        b_rows = pl.ds(pl.multiple_of(b_row + block * BLOCK_LEN, BLOCK_LEN), BLOCK_LEN)
        for h in range(n_heads):
            w_s[a_rows, head(h)] = jnp.where(causal, dot_nt(q_of(rows, h), k_of(rows, h)), 0.0).astype(BF16)
            w_s[b_rows, head(h)] = jnp.where(causal, dot_nt(do_of(rows, h), v_of(rows, h)), 0.0).astype(BF16)

    def spread(first_tick, stride):
        def extra(step):
            @pl.when(lax.rem(step, stride) == 0)
            def _():
                chain_s(first_tick + lax.div(step, stride))

        return extra

    accumulate(q_of, do_of, qdo_slot, r_out, True, spread(tick_r, stride_r))

    @pl.when(chip == n_chips - 1)
    def _():
        for h in range(n_heads):
            chain_r(h)

    score_ticks = spread(tick_scores, stride_scores)

    @pl.loop(0, n_blocks)
    def _(block):
        score_ticks(block)
        block_scores(block)

    def scores(block, h):
        a_rows = pl.ds(pl.multiple_of(a_row + block * BLOCK_LEN, BLOCK_LEN), BLOCK_LEN)
        b_rows = pl.ds(pl.multiple_of(b_row + block * BLOCK_LEN, BLOCK_LEN), BLOCK_LEN)
        return w_s[a_rows, head(h)], w_s[b_rows, head(h)]

    def both(left, right, top, bottom):
        out = dot(jnp.concatenate([left, right], axis=1), jnp.concatenate([top, bottom], axis=0))
        return (out * scale).astype(BF16)

    group = 4

    @pl.loop(0, n_heads)
    def _(h):
        @pl.when(chip == n_chips - 2)
        def _():
            chain_r(h)

        @pl.when(odd == 0)
        def _():
            even_s(h)

        @pl.when((odd == 1) & (due + h >= last_tick))
        def _():
            odd_s(h)

        @pl.loop(0, n_blocks // group)
        def _(part):
            for inner in range(group):
                block = part * group + inner
                rows = aligned(block, BLOCK_LEN)
                a, b = scores(block, h)
                s = (s_in[h] + grads[kv_slot + block, :, head(h)]).astype(BF16)
                xo[rows, head(h, dim)] = both(a, q_of(rows, h), v_of(rows, h), s)
                ra[rows, head(h)] = both(b, do_of(rows, h), k_of(rows, h), s.T)

    def rev_block(block):
        rows = aligned(block, BLOCK_LEN)
        for h in range(n_heads):
            a, b = scores(block, h)
            r = (r_in[h] + grads[qdo_slot + block, :, head(h)]).astype(BF16)
            dk = both(b.T, v_of(rows, h), q_of(rows, h), r.T)
            dv = both(a.T, k_of(rows, h), do_of(rows, h), r)
            ra[rows, head(h, k_col)] = dk
            ra[rows, head(h, v_col)] = dv

    def credit(which):
        pl.semaphore_signal(credits.at[which], inc=1, device_id={"sp": previous}, device_id_type=MESH)

    def term(late, unit):
        inside, second = lax.rem(unit, per_weight), lax.div(unit, per_weight)
        if late:
            left, right = inside, 3 + second
        else:
            left = (1 - second) * inside + second * (per_weight + lax.div(inside, 2))
            right = second * (1 + lax.rem(inside, 2))
        return dot_t(xo[:, aligned(left, TILE)], ra[:, aligned(right, width)])

    def unit_of(step, piece):
        return lax.rem(rank - step + n_chips, n_chips) * early + piece

    def hop(late, step, piece):
        slot = grads.at[late * (n_slots // 2) + unit_of(step, piece)]
        sems = send_sems.at[late, step, piece], recv_sems.at[late, step, piece]
        return slot, sems

    def start_hop(late, step, piece, first):
        slot, sems = hop(late, step, piece)
        send(slot, land.at[late * early + piece] if first else slot, *sems, following).start()

    def run_ring(late, extra):
        offset = late * (n_slots // 2)

        @pl.loop(0, early)
        def _(piece):
            unit = unit_of(0, piece)
            grads[offset + unit] = term(late, unit)
            start_hop(late, 0, piece, True)

        @pl.loop(0, (n_chips - 1) * early)
        def _(index):
            step, piece = lax.div(index, early) + 1, lax.rem(index, early)
            unit = unit_of(step, piece)
            slot = offset + unit
            extra(index)
            mine = term(late, unit)

            @pl.when(step == 1)
            def _():
                place = land.at[late * early + piece]
                send(place, place, send_sems.at[late, 0, piece], recv_sems.at[late, 0, piece], following).wait_recv()
                grads[slot] = place[...] + mine

            @pl.when(step > 1)
            def _():
                place = grads.at[slot]
                send(place, place, send_sems.at[late, step - 1, piece], recv_sems.at[late, step - 1, piece], following).wait_recv()
                grads[slot] = grads[slot] + mine

            @pl.when(index == 0)
            def _():
                pl.semaphore_wait(credits.at[late], 1)

            @pl.when(step < n_chips - 1)
            def _():
                start_hop(late, step, piece, False)

            @pl.when(step == n_chips - 1)
            def _():
                pltpu.make_async_copy(grads.at[slot], red_out.at[late * early + piece], red_sems.at[late * early + piece]).start()

    share = n_blocks // 4

    def reverse_work(index):
        @pl.when(((index == n_chips // 2 - chip) | ((index == 0) & (chip > n_chips // 2))) & (chip < n_chips - 2))
        def _():
            for h in range(n_heads):
                chain_r(h)

        @pl.when((index > n_chips) & (index <= n_chips + 4))
        def _():
            @pl.loop(0, share)
            def _(part):
                rev_block((index - n_chips - 1) * share + part)

        @pl.when(index == n_chips + 4)
        def _():
            credit(1)

    credit(0)
    run_ring(0, reverse_work)

    copies = []
    for index, (src, column) in enumerate(((xo, dim), (ra, 0), (ra, k_col), (ra, v_col))):
        part = pl.ds(column, width)
        copies.append(pltpu.make_async_copy(src.at[own_rows, part], own_out.at[index, :, w_cols], own_sems.at[index, 0]))
        copies.append(send(src.at[peer_rows, part], own_out.at[index, :, w_cols], own_sems.at[index, 1], own_sems.at[index, 2], peer))
    for copy in copies:
        copy.start()

    run_ring(1, lambda index: None)

    sent = ((EVEN, odd == 0), (PAIR, (odd == 1) & (chip + 2 < n_chips)), (HAND, (odd == 1) & (chip > 1)), (REV, chip > 0))
    for which, sends in sent:
        @pl.when(sends)
        def _():
            for h in range(n_heads):
                chain_copy(which, h).wait_send()

    for late in range(2):
        @pl.loop(0, (n_chips - 1) * early)
        def _(index):
            step, piece = lax.div(index, early), lax.rem(index, early)
            slot, sems = hop(late, step, piece)
            send(slot, slot, *sems, following).wait_send()

    for copy in copies:
        copy.wait()
    for late in range(2):
        for piece in range(early):
            slot = late * (n_slots // 2) + lax.rem(rank + 1, n_chips) * early + piece
            pltpu.make_async_copy(grads.at[slot], red_out.at[late * early + piece], red_sems.at[late * early + piece]).wait()


def tile_slot(chunk, piece, early):
    return chunk * early + lax.rem(piece, early), lax.div(piece, early)


def gather_kernel(n_seq, red, own, wq, wk, wv, wo, rows_out, both_out, own_s, wo_s, w_s, own_sems, w_sems, send_sems, recv_sems, peer_sems):
    core, rank, n_chips, peer, following, previous = ring(n_seq)
    mine_out, peer_out = both_out.at[0], both_out.at[1]
    y_out, dx_out = rows_out.at[0], rows_out.at[1]
    n_slots, _, width = mine_out.shape
    dim = 2 * width
    early = 2 * (dim // TILE) // n_chips
    pieces = 2 * early
    n_rows = own.shape[1]
    unit_cols = wo_s.shape[2]
    n_units = dim // unit_cols
    row_blocks = n_rows // ROWS

    def slot_of(chunk, piece):
        unit, late = tile_slot(chunk, piece, early)
        return unit + late * (n_slots // 2)

    def held(step, piece):
        return slot_of(lax.rem(rank + 1 - step + n_chips, n_chips), piece)

    def w_loads(unit, buffer):
        part = aligned(unit, unit_cols)
        loads = [pltpu.make_async_copy(wo.at[:, part], wo_s.at[buffer], w_sems.at[buffer, 0])]
        for index, weight in enumerate((wq, wk, wv)):
            loads.append(pltpu.make_async_copy(weight.at[part], w_s.at[buffer, index], w_sems.at[buffer, 1 + index]))
        return loads

    own_load = pltpu.make_async_copy(own, own_s, own_sems.at[0])
    own_load.start()
    for unit in range(2):
        for load in w_loads(unit, unit):
            load.start()
    red_loads = [pltpu.make_async_copy(red.at[piece], mine_out.at[held(0, piece)], own_sems.at[1 + piece]) for piece in range(pieces)]
    for load in red_loads:
        load.start()

    entry_barrier((peer, following, previous))

    def to_next(step, piece):
        slot = held(step, piece)
        return send(mine_out.at[slot], mine_out.at[slot], send_sems.at[step, piece], recv_sems.at[step, piece], following)

    def arrival(step, piece):
        slot = held(step + 1, piece)
        return send(mine_out.at[slot], mine_out.at[slot], send_sems.at[step, piece], recv_sems.at[step, piece], following)

    def to_peer(step, piece):
        slot = held(step, piece)
        return send(mine_out.at[slot], peer_out.at[slot], peer_sems.at[0, step, piece], peer_sems.at[1, step, piece], peer)

    for piece in range(pieces):
        red_loads[piece].wait()
        to_next(0, piece).start()
        to_peer(0, piece).start()
    own_load.wait()

    def project(unit, block):
        buffer = lax.rem(unit, 2)

        @pl.when(block == 0)
        def _():
            for load in w_loads(unit, buffer):
                load.wait()

        rows, cols = aligned(block, ROWS), aligned(unit, unit_cols)
        y_out[rows, cols] = dot(own_s[0, rows, :], wo_s[buffer]).astype(BF16)
        total = dot_nt(own_s[1, rows, :], w_s[buffer, 0])
        total += dot_nt(own_s[2, rows, :], w_s[buffer, 1])
        total += dot_nt(own_s[3, rows, :], w_s[buffer, 2])
        dx_out[rows, cols] = total.astype(BF16)

        @pl.when((block == row_blocks - 1) & (unit + 2 < n_units))
        def _():
            for load in w_loads(unit + 2, buffer):
                load.start()

    @pl.loop(0, (n_chips - 1) * pieces)
    def _(index):
        step, piece = lax.div(index, pieces), lax.rem(index, pieces)

        @pl.when(index < n_units * row_blocks)
        def _():
            project(lax.div(index, row_blocks), lax.rem(index, row_blocks))

        arrival(step, piece).wait_recv()

        @pl.when(step < n_chips - 2)
        def _():
            to_next(step + 1, piece).start()

        to_peer(step + 1, piece).start()

    @pl.loop(0, n_chips * pieces)
    def _(index):
        step, piece = lax.div(index, pieces), lax.rem(index, pieces)

        @pl.when(step < n_chips - 1)
        def _():
            to_next(step, piece).wait_send()

        to_peer(step, piece).wait()


def place_kernel(results, both, y, dx, gq, gk, gv, go, sems):
    core = lax.rem(lax.axis_index("sp"), 2)
    _, n_slots, _, width = both.shape
    per_weight = n_slots // 4
    copies = [pltpu.make_async_copy(results.at[0], y, sems.at[2]), pltpu.make_async_copy(results.at[1], dx, sems.at[3])]
    for side, half in enumerate((core, 1 - core)):
        cols = aligned(half, width)
        for slot in range(n_slots):
            weight, inside = slot // per_weight, slot % per_weight
            if weight == 1:
                rows = pl.ds(pl.multiple_of(half * width + inside // 2 * TILE, TILE), TILE)
                dst = go.at[rows, pl.ds(inside % 2 * width, width)]
            else:
                dst = (gq, None, gk, gv)[weight].at[pl.ds(inside * TILE, TILE), cols]
            copies.append(pltpu.make_async_copy(both.at[side, slot], dst, sems.at[side]))
    for copy in copies:
        copy.start()
    for copy in copies:
        copy.wait()


def solution(mesh):
    n_seq = mesh.shape["sp"]
    n_chips = n_seq // 2
    row_spec = P(("dp", "sp"), None)
    grad_spec = P("dp", None)
    any_spec = pl.BlockSpec(memory_space=pl.ANY)
    vmem_spec = pl.BlockSpec(memory_space=pltpu.VMEM)
    dma = pltpu.SemaphoreType.DMA

    def params(collective_id, limit=VMEM_LIMIT):
        return pltpu.CompilerParams(collective_id=collective_id, has_side_effects=True, vmem_limit_bytes=limit)

    def local_layer(tokens, w_q, w_k, w_v, w_o, grad_y):
        n_rows, dim = tokens.shape
        width = dim // 2
        n_heads = width // HEAD_DIM
        rows = 2 * n_rows
        n_slots = 4 * (dim // TILE)
        pieces = n_slots // n_chips
        scale = 1.0 / math.sqrt(n_rows * n_seq * HEAD_DIM)
        state = (n_heads, HEAD_DIM, HEAD_DIM)

        own, red = pl.pallas_call(
            functools.partial(attention_kernel, n_seq, scale),
            out_shape=(jax.ShapeDtypeStruct((4, n_rows, dim), BF16), jax.ShapeDtypeStruct((pieces, TILE, width), F32)),
            in_specs=[any_spec] * 6,
            out_specs=(any_spec,) * 2,
            scratch_shapes=[pltpu.VMEM((rows, dim + width), BF16), pltpu.VMEM((rows, dim + 3 * width), BF16), pltpu.VMEM((4 * dim, width), BF16)]
            + [pltpu.VMEM((rows, width), BF16)] * 2
            + [pltpu.VMEM((n_slots, TILE, width), F32), pltpu.VMEM((pieces, TILE, width), F32)]
            + [pltpu.VMEM(state, F32)] * 6
            + [dma((2, 3)), dma((5,)), dma((4, 2, n_heads))]
            + [dma((2, n_chips - 1, pieces // 2))] * 2
            + [dma((4, 3)), dma((pieces,)), pltpu.SemaphoreType.REGULAR((2,))],
            compiler_params=params(0),
            name="attention",
        )(tokens, grad_y, w_q, w_k, w_v, w_o)

        unit_cols = min(256, dim // 2)
        halves = (2, n_slots, TILE, width)
        room = VMEM_LIMIT - math.prod(halves) * 4 - 4 * n_rows * dim - (1 << 20)
        results = pl.pallas_call(
            functools.partial(gather_kernel, n_seq),
            out_shape=(pltpu.VMEM((2, n_rows, dim), BF16), pltpu.VMEM(halves, F32)),
            in_specs=[any_spec] * 6,
            out_specs=(vmem_spec,) * 2,
            scratch_shapes=[pltpu.VMEM((4, n_rows, dim), BF16), pltpu.VMEM((2, dim, unit_cols), BF16), pltpu.VMEM((2, 3, unit_cols, dim), BF16)]
            + [dma((1 + pieces,)), dma((2, 4)), dma((n_chips - 1, pieces)), dma((n_chips - 1, pieces)), dma((2, n_chips, pieces))],
            compiler_params=params(1, room),
            name="gather",
        )(red, own, w_q, w_k, w_v, w_o)

        return pl.pallas_call(
            place_kernel,
            out_shape=(jax.ShapeDtypeStruct((n_rows, dim), BF16),) * 2 + (jax.ShapeDtypeStruct((dim, dim), F32),) * 4,
            in_specs=[vmem_spec] * 2,
            out_specs=(any_spec,) * 6,
            scratch_shapes=[dma((4,))],
            compiler_params=pltpu.CompilerParams(vmem_limit_bytes=1 << 20),
            name="place",
        )(*results)

    return jax.shard_map(local_layer, mesh=mesh, in_specs=(row_spec, P(), P(), P(), P(), row_spec), out_specs=(row_spec, row_spec, grad_spec, grad_spec, grad_spec, grad_spec), check_vma=False)
```

```python
import functools
import math
import jax
import jax.numpy as jnp
from jax import lax
from jax.experimental import pallas as pl
from jax.experimental.pallas import tpu as pltpu
from jax.sharding import PartitionSpec as P

HEAD_DIM = 128
BLOCK_LEN = 128
TILE = 128
ROWS = 256
MESH = pl.DeviceIdType.MESH
VMEM_LIMIT = 67_043_328
F32 = jnp.float32
BF16 = jnp.bfloat16


def dot_t(lhs, rhs):
    return lax.dot_general(lhs, rhs, (((0,), (0,)), ((), ())), preferred_element_type=F32)


def dot_nt(lhs, rhs):
    return lax.dot_general(lhs, rhs, (((1,), (1,)), ((), ())), preferred_element_type=F32)


def dot(lhs, rhs):
    return jnp.dot(lhs, rhs, preferred_element_type=F32)


def aligned(index, size):
    return pl.ds(pl.multiple_of(index * size, size), size)


def position(n_seq):
    me = lax.axis_index("sp")
    core, chip = lax.rem(me, 2), lax.div(me, 2)
    return core, chip, n_seq // 2, me + 1 - 2 * core


def send(src, dst, send_sem, recv_sem, target):
    return pltpu.make_async_remote_copy(src_ref=src, dst_ref=dst, send_sem=send_sem, recv_sem=recv_sem, device_id={"sp": target}, device_id_type=MESH)


def entry_barrier(targets):
    barrier = pltpu.get_barrier_semaphore()
    for target in targets:
        pl.semaphore_signal(barrier, inc=1, device_id={"sp": target}, device_id_type=MESH)
    pl.semaphore_wait(barrier, len(targets))


def ring(n_seq):
    core, chip, n_chips, peer = position(n_seq)
    me = lax.axis_index("sp")
    rank = (1 - core) * chip + core * lax.rem(n_chips - chip, n_chips)
    following = lax.rem(me + 2 - 4 * core + n_seq, n_seq)
    previous = lax.rem(me - 2 + 4 * core + n_seq, n_seq)
    return core, rank, n_chips, peer, following, previous


def attention_kernel(n_seq, scale, x, dy, wq, wk, wv, wo, own_out, red_out, xo, ra, w_s, q, do, grads, land, s_in, s_out, s_even, s_pair, r_in, r_out, x_sems, w_sems, chain_sems, send_sems, recv_sems, own_sems, red_sems, credits):
    _, chip, _, _ = position(n_seq)
    core, rank, n_chips, peer, following, previous = ring(n_seq)
    me = lax.axis_index("sp")
    up, down = lax.rem(me + 2, n_seq), lax.rem(me + n_seq - 2, n_seq)
    up_two, down_two = lax.rem(me + 4, n_seq), lax.rem(me + n_seq - 4, n_seq)
    n_rows, dim = x.shape
    all_rows, width = q.shape
    n_heads = width // HEAD_DIM
    n_blocks = all_rows // BLOCK_LEN
    n_slots = grads.shape[0]
    per_weight = dim // TILE
    early = 2 * per_weight // n_chips
    own_rows, peer_rows = aligned(core, n_rows), aligned(1 - core, n_rows)
    w_cols = aligned(core, width)
    k_col, v_col, a_row, b_row = width + dim, 2 * width + dim, 0, all_rows
    kv_slot, qdo_slot = 0, n_slots // 2

    entry_barrier((peer, up, down, up_two, down_two))
    x_part, dy_part = pl.ds(0, dim), pl.ds(width, dim)
    local, remote = [], []
    for index, (src, dst) in enumerate(((x, xo.at[own_rows, x_part]), (dy, ra.at[own_rows, dy_part]))):
        remote.append(send(src, dst, x_sems.at[index, 0], x_sems.at[index, 1], peer))
        local.append(pltpu.make_async_copy(src, dst, x_sems.at[index, 2]))
    w_loads = [pltpu.make_async_copy(weight.at[:, w_cols], w_s.at[pl.ds(index * dim, dim)], w_sems.at[index]) for index, weight in enumerate((wk, wv, wq))]
    for part in range(2):
        w_loads.append(pltpu.make_async_copy(wo.at[w_cols, pl.ds(part * width, width)], w_s.at[pl.ds(3 * dim + part * width, width)], w_sems.at[3 + part]))
    remote[0].start()
    local[0].start()
    for load in w_loads[:2]:
        load.start()
    remote[1].start()
    for load in w_loads[2:]:
        load.start()
    local[1].start()

    def weight(index, size):
        return w_s[pl.ds(index * size, size), :]

    def part_rows(half, step):
        return pl.ds(pl.multiple_of(half * n_rows + step * ROWS, ROWS), ROWS)

    def project_kv(half):
        @pl.loop(0, n_rows // ROWS)
        def _(step):
            rows = part_rows(half, step)
            ra[rows, pl.ds(k_col, width)] = dot(xo[rows, x_part], weight(0, dim)).astype(BF16)
            ra[rows, pl.ds(v_col, width)] = dot(xo[rows, x_part], weight(1, dim)).astype(BF16)

    local[0].wait()
    w_loads[0].wait()
    w_loads[1].wait()
    project_kv(core)
    remote[0].wait()
    project_kv(1 - core)

    def head(h, column=0):
        return pl.ds(pl.multiple_of(column + h * HEAD_DIM, HEAD_DIM), HEAD_DIM)

    def accumulate(left, right, slot, total, reverse, extra):
        total[...] = jnp.zeros_like(total)

        @pl.loop(0, n_blocks)
        def _(step):
            block = (n_blocks - 1 - step) if reverse else step
            rows = aligned(block, BLOCK_LEN)
            extra(step)
            for h in range(n_heads):
                running = total[h]
                grads[slot + block, :, head(h)] = running
                total[h] = running + dot_t(left(rows, h), right(rows, h))

    def q_of(rows, h):
        return q[rows, head(h)]

    def do_of(rows, h):
        return do[rows, head(h)]

    def k_of(rows, h):
        return ra[rows, head(h, k_col)]

    def v_of(rows, h):
        return ra[rows, head(h, v_col)]

    odd = lax.rem(chip, 2)
    EVEN, PAIR, HAND, REV = range(4)

    def chain_copy(which, h):
        src, dst, target = ((s_out, s_even, up), (s_out, s_pair, up_two), (s_pair, s_in, down), (r_out, r_in, down))[which]
        return send(src.at[h], dst.at[h], chain_sems.at[which, 0, h], chain_sems.at[which, 1, h], target)

    def start_s():
        @pl.when(odd == 0)
        def _():
            for h in range(n_heads):
                chain_copy(EVEN, h).start()

    def odd_s(h):
        chain_copy(EVEN, h).wait_recv()

        @pl.when(chip == 1)
        def _():
            s_in[h] = s_even[h]

        @pl.when(chip != 1)
        def _():
            chain_copy(PAIR, h).wait_recv()
            chain_copy(HAND, h).start()
            s_in[h] = s_pair[h] + s_even[h]

        @pl.when(chip + 2 < n_chips)
        def _():
            s_out[h] = s_out[h] + s_in[h]
            chain_copy(PAIR, h).start()

    def even_s(h):
        @pl.when(chip == 0)
        def _():
            s_in[h] = jnp.zeros_like(s_in[h])

        @pl.when(chip != 0)
        def _():
            chain_copy(HAND, h).wait_recv()

    def chain_r(h):
        @pl.when(chip == n_chips - 1)
        def _():
            r_in[h] = jnp.zeros_like(r_in[h])

        @pl.when(chip != n_chips - 1)
        def _():
            chain_copy(REV, h).wait_recv()
            r_out[h] = r_out[h] + r_in[h]

        @pl.when(chip != 0)
        def _():
            chain_copy(REV, h).start()

    steps = n_rows // ROWS
    due = 3 + lax.div(7 * lax.div(chip, 2), 2)
    stride_r, stride_scores = n_blocks // 2, -(-n_blocks // 3)
    tick_r, tick_scores = 2 * steps, 2 * steps + 2
    last_tick = tick_scores + -(-n_blocks // stride_scores)

    def chain_s(tick):
        @pl.when((odd == 1) & (tick >= due) & (tick < due + n_heads))
        def _():
            odd_s(tick - due)

    accumulate(k_of, v_of, kv_slot, s_out, False, lambda step: None)
    start_s()

    def project_qdo(half, first_tick):
        @pl.loop(0, steps)
        def _(step):
            chain_s(first_tick + step)
            rows = part_rows(half, step)
            q[rows, :] = dot(xo[rows, x_part], weight(2, dim)).astype(BF16)
            product = dot_nt(ra[rows, pl.ds(width, width)], weight(6, width))
            product += dot_nt(ra[rows, pl.ds(2 * width, width)], weight(7, width))
            do[rows, :] = product.astype(BF16)

    for load in w_loads[2:] + [local[1]]:
        load.wait()
    project_qdo(core, 0)
    remote[1].wait()
    project_qdo(1 - core, steps)

    causal = lax.broadcasted_iota(jnp.int32, (BLOCK_LEN, BLOCK_LEN), 0) >= lax.broadcasted_iota(jnp.int32, (BLOCK_LEN, BLOCK_LEN), 1)

    def block_scores(block):
        rows = aligned(block, BLOCK_LEN)
        a_rows = pl.ds(pl.multiple_of(a_row + block * BLOCK_LEN, BLOCK_LEN), BLOCK_LEN)
        b_rows = pl.ds(pl.multiple_of(b_row + block * BLOCK_LEN, BLOCK_LEN), BLOCK_LEN)
        for h in range(n_heads):
            w_s[a_rows, head(h)] = jnp.where(causal, dot_nt(q_of(rows, h), k_of(rows, h)), 0.0).astype(BF16)
            w_s[b_rows, head(h)] = jnp.where(causal, dot_nt(do_of(rows, h), v_of(rows, h)), 0.0).astype(BF16)

    def spread(first_tick, stride):
        def extra(step):
            @pl.when(lax.rem(step, stride) == 0)
            def _():
                chain_s(first_tick + lax.div(step, stride))

        return extra

    accumulate(q_of, do_of, qdo_slot, r_out, True, spread(tick_r, stride_r))

    score_ticks = spread(tick_scores, stride_scores)

    @pl.loop(0, n_blocks)
    def _(block):
        score_ticks(block)
        block_scores(block)

    def scores(block, h):
        a_rows = pl.ds(pl.multiple_of(a_row + block * BLOCK_LEN, BLOCK_LEN), BLOCK_LEN)
        b_rows = pl.ds(pl.multiple_of(b_row + block * BLOCK_LEN, BLOCK_LEN), BLOCK_LEN)
        return w_s[a_rows, head(h)], w_s[b_rows, head(h)]

    def both(left, right, top, bottom):
        out = dot(jnp.concatenate([left, right], axis=1), jnp.concatenate([top, bottom], axis=0))
        return (out * scale).astype(BF16)

    group = 4

    @pl.loop(0, n_heads)
    def _(h):
        @pl.when(odd == 0)
        def _():
            even_s(h)

        @pl.when((odd == 1) & (due + h >= last_tick))
        def _():
            odd_s(h)

        @pl.loop(0, n_blocks // group)
        def _(part):
            for inner in range(group):
                block = part * group + inner
                rows = aligned(block, BLOCK_LEN)
                a, b = scores(block, h)
                s = (s_in[h] + grads[kv_slot + block, :, head(h)]).astype(BF16)
                xo[rows, head(h, dim)] = both(a, q_of(rows, h), v_of(rows, h), s)
                ra[rows, head(h)] = both(b, do_of(rows, h), k_of(rows, h), s.T)

    def rev_head(h):
        @pl.loop(0, n_blocks // group)
        def _(part):
            for inner in range(group):
                block = part * group + inner
                rows = aligned(block, BLOCK_LEN)
                a, b = scores(block, h)
                r = (r_in[h] + grads[qdo_slot + block, :, head(h)]).astype(BF16)
                dk = both(b.T, v_of(rows, h), q_of(rows, h), r.T)
                dv = both(a.T, k_of(rows, h), do_of(rows, h), r)
                ra[rows, head(h, k_col)] = dk
                ra[rows, head(h, v_col)] = dv

    def credit(which):
        pl.semaphore_signal(credits.at[which], inc=1, device_id={"sp": previous}, device_id_type=MESH)

    def term(late, unit):
        inside, second = lax.rem(unit, per_weight), lax.div(unit, per_weight)
        if late:
            left, right = inside, 3 + second
        else:
            left = (1 - second) * inside + second * (per_weight + lax.div(inside, 2))
            right = second * (1 + lax.rem(inside, 2))
        return dot_t(xo[:, aligned(left, TILE)], ra[:, aligned(right, width)])

    def unit_of(step, piece):
        return lax.rem(rank - step + n_chips, n_chips) * early + piece

    def hop(late, step, piece):
        slot = grads.at[late * (n_slots // 2) + unit_of(step, piece)]
        sems = send_sems.at[late, step, piece], recv_sems.at[late, step, piece]
        return slot, sems

    def start_hop(late, step, piece, first):
        slot, sems = hop(late, step, piece)
        send(slot, land.at[late * early + piece] if first else slot, *sems, following).start()

    def run_ring(late, extra):
        offset = late * (n_slots // 2)

        @pl.loop(0, early)
        def _(piece):
            unit = unit_of(0, piece)
            grads[offset + unit] = term(late, unit)
            start_hop(late, 0, piece, True)

        @pl.loop(0, (n_chips - 1) * early)
        def _(index):
            step, piece = lax.div(index, early) + 1, lax.rem(index, early)
            unit = unit_of(step, piece)
            slot = offset + unit
            extra(index)
            mine = term(late, unit)

            @pl.when(step == 1)
            def _():
                place = land.at[late * early + piece]
                send(place, place, send_sems.at[late, 0, piece], recv_sems.at[late, 0, piece], following).wait_recv()
                grads[slot] = place[...] + mine

            @pl.when(step > 1)
            def _():
                place = grads.at[slot]
                send(place, place, send_sems.at[late, step - 1, piece], recv_sems.at[late, step - 1, piece], following).wait_recv()
                grads[slot] = grads[slot] + mine

            @pl.when(index == 0)
            def _():
                pl.semaphore_wait(credits.at[late], 1)

            @pl.when(step < n_chips - 1)
            def _():
                start_hop(late, step, piece, False)

            @pl.when(step == n_chips - 1)
            def _():
                pltpu.make_async_copy(grads.at[slot], red_out.at[late * early + piece], red_sems.at[late * early + piece]).start()

    stride = ((n_chips - 1) * early - n_heads) // (n_chips - 1)
    rev_start = stride * (n_chips - 1 - chip)

    def reverse_work(index):
        @pl.when((index >= rev_start) & (index < rev_start + n_heads))
        def _():
            chain_r(index - rev_start)
            rev_head(index - rev_start)

        @pl.when(index == rev_start + n_heads - 1)
        def _():
            credit(1)

    credit(0)
    run_ring(0, reverse_work)

    copies = []
    for index, (src, column) in enumerate(((xo, dim), (ra, 0), (ra, k_col), (ra, v_col))):
        part = pl.ds(column, width)
        copies.append(pltpu.make_async_copy(src.at[own_rows, part], own_out.at[index, :, w_cols], own_sems.at[index, 0]))
        copies.append(send(src.at[peer_rows, part], own_out.at[index, :, w_cols], own_sems.at[index, 1], own_sems.at[index, 2], peer))
    for copy in copies:
        copy.start()

    run_ring(1, lambda index: None)

    sent = ((EVEN, odd == 0), (PAIR, (odd == 1) & (chip + 2 < n_chips)), (HAND, (odd == 1) & (chip > 1)), (REV, chip > 0))
    for which, sends in sent:
        @pl.when(sends)
        def _():
            for h in range(n_heads):
                chain_copy(which, h).wait_send()

    for late in range(2):
        @pl.loop(0, (n_chips - 1) * early)
        def _(index):
            step, piece = lax.div(index, early), lax.rem(index, early)
            slot, sems = hop(late, step, piece)
            send(slot, slot, *sems, following).wait_send()

    for copy in copies:
        copy.wait()
    for late in range(2):
        for piece in range(early):
            slot = late * (n_slots // 2) + lax.rem(rank + 1, n_chips) * early + piece
            pltpu.make_async_copy(grads.at[slot], red_out.at[late * early + piece], red_sems.at[late * early + piece]).wait()


def tile_slot(chunk, piece, early):
    return chunk * early + lax.rem(piece, early), lax.div(piece, early)


def gather_kernel(n_seq, red, own, wq, wk, wv, wo, rows_out, both_out, own_s, wo_s, w_s, own_sems, w_sems, send_sems, recv_sems, peer_sems):
    core, rank, n_chips, peer, following, previous = ring(n_seq)
    mine_out, peer_out = both_out.at[0], both_out.at[1]
    y_out, dx_out = rows_out.at[0], rows_out.at[1]
    n_slots, _, width = mine_out.shape
    dim = 2 * width
    early = 2 * (dim // TILE) // n_chips
    pieces = 2 * early
    n_rows = own.shape[1]
    unit_cols = wo_s.shape[2]
    n_units = dim // unit_cols
    row_blocks = n_rows // ROWS

    def slot_of(chunk, piece):
        unit, late = tile_slot(chunk, piece, early)
        return unit + late * (n_slots // 2)

    def held(step, piece):
        return slot_of(lax.rem(rank + 1 - step + n_chips, n_chips), piece)

    def w_loads(unit, buffer):
        part = aligned(unit, unit_cols)
        loads = [pltpu.make_async_copy(wo.at[:, part], wo_s.at[buffer], w_sems.at[buffer, 0])]
        for index, weight in enumerate((wq, wk, wv)):
            loads.append(pltpu.make_async_copy(weight.at[part], w_s.at[buffer, index], w_sems.at[buffer, 1 + index]))
        return loads

    own_load = pltpu.make_async_copy(own, own_s, own_sems.at[0])
    own_load.start()
    for unit in range(2):
        for load in w_loads(unit, unit):
            load.start()
    red_loads = [pltpu.make_async_copy(red.at[piece], mine_out.at[held(0, piece)], own_sems.at[1 + piece]) for piece in range(pieces)]
    for load in red_loads:
        load.start()

    entry_barrier((peer, following, previous))

    def to_next(step, piece):
        slot = held(step, piece)
        return send(mine_out.at[slot], mine_out.at[slot], send_sems.at[step, piece], recv_sems.at[step, piece], following)

    def arrival(step, piece):
        slot = held(step + 1, piece)
        return send(mine_out.at[slot], mine_out.at[slot], send_sems.at[step, piece], recv_sems.at[step, piece], following)

    def to_peer(step, piece):
        slot = held(step, piece)
        return send(mine_out.at[slot], peer_out.at[slot], peer_sems.at[0, step, piece], peer_sems.at[1, step, piece], peer)

    for piece in range(pieces):
        red_loads[piece].wait()
        to_next(0, piece).start()
        to_peer(0, piece).start()
    own_load.wait()

    def project(unit, block):
        buffer = lax.rem(unit, 2)

        @pl.when(block == 0)
        def _():
            for load in w_loads(unit, buffer):
                load.wait()

        rows, cols = aligned(block, ROWS), aligned(unit, unit_cols)
        y_out[rows, cols] = dot(own_s[0, rows, :], wo_s[buffer]).astype(BF16)
        total = dot_nt(own_s[1, rows, :], w_s[buffer, 0])
        total += dot_nt(own_s[2, rows, :], w_s[buffer, 1])
        total += dot_nt(own_s[3, rows, :], w_s[buffer, 2])
        dx_out[rows, cols] = total.astype(BF16)

        @pl.when((block == row_blocks - 1) & (unit + 2 < n_units))
        def _():
            for load in w_loads(unit + 2, buffer):
                load.start()

    @pl.loop(0, (n_chips - 1) * pieces)
    def _(index):
        step, piece = lax.div(index, pieces), lax.rem(index, pieces)

        @pl.when(index < n_units * row_blocks)
        def _():
            project(lax.div(index, row_blocks), lax.rem(index, row_blocks))

        arrival(step, piece).wait_recv()

        @pl.when(step < n_chips - 2)
        def _():
            to_next(step + 1, piece).start()

        to_peer(step + 1, piece).start()

    @pl.loop(0, n_chips * pieces)
    def _(index):
        step, piece = lax.div(index, pieces), lax.rem(index, pieces)

        @pl.when(step < n_chips - 1)
        def _():
            to_next(step, piece).wait_send()

        to_peer(step, piece).wait()


def place_kernel(results, both, y, dx, gq, gk, gv, go, sems):
    core = lax.rem(lax.axis_index("sp"), 2)
    _, n_slots, _, width = both.shape
    per_weight = n_slots // 4
    copies = [pltpu.make_async_copy(results.at[0], y, sems.at[2]), pltpu.make_async_copy(results.at[1], dx, sems.at[3])]
    for side, half in enumerate((core, 1 - core)):
        cols = aligned(half, width)
        for slot in range(n_slots):
            weight, inside = slot // per_weight, slot % per_weight
            if weight == 1:
                rows = pl.ds(pl.multiple_of(half * width + inside // 2 * TILE, TILE), TILE)
                dst = go.at[rows, pl.ds(inside % 2 * width, width)]
            else:
                dst = (gq, None, gk, gv)[weight].at[pl.ds(inside * TILE, TILE), cols]
            copies.append(pltpu.make_async_copy(both.at[side, slot], dst, sems.at[side]))
    for copy in copies:
        copy.start()
    for copy in copies:
        copy.wait()


def solution(mesh):
    n_seq = mesh.shape["sp"]
    n_chips = n_seq // 2
    row_spec = P(("dp", "sp"), None)
    grad_spec = P("dp", None)
    any_spec = pl.BlockSpec(memory_space=pl.ANY)
    vmem_spec = pl.BlockSpec(memory_space=pltpu.VMEM)
    dma = pltpu.SemaphoreType.DMA

    def params(collective_id, limit=VMEM_LIMIT):
        return pltpu.CompilerParams(collective_id=collective_id, has_side_effects=True, vmem_limit_bytes=limit)

    def local_layer(tokens, w_q, w_k, w_v, w_o, grad_y):
        n_rows, dim = tokens.shape
        width = dim // 2
        n_heads = width // HEAD_DIM
        rows = 2 * n_rows
        n_slots = 4 * (dim // TILE)
        pieces = n_slots // n_chips
        scale = 1.0 / math.sqrt(n_rows * n_seq * HEAD_DIM)
        state = (n_heads, HEAD_DIM, HEAD_DIM)

        own, red = pl.pallas_call(
            functools.partial(attention_kernel, n_seq, scale),
            out_shape=(jax.ShapeDtypeStruct((4, n_rows, dim), BF16), jax.ShapeDtypeStruct((pieces, TILE, width), F32)),
            in_specs=[any_spec] * 6,
            out_specs=(any_spec,) * 2,
            scratch_shapes=[pltpu.VMEM((rows, dim + width), BF16), pltpu.VMEM((rows, dim + 3 * width), BF16), pltpu.VMEM((4 * dim, width), BF16)]
            + [pltpu.VMEM((rows, width), BF16)] * 2
            + [pltpu.VMEM((n_slots, TILE, width), F32), pltpu.VMEM((pieces, TILE, width), F32)]
            + [pltpu.VMEM(state, F32)] * 6
            + [dma((2, 3)), dma((5,)), dma((4, 2, n_heads))]
            + [dma((2, n_chips - 1, pieces // 2))] * 2
            + [dma((4, 3)), dma((pieces,)), pltpu.SemaphoreType.REGULAR((2,))],
            compiler_params=params(0),
            name="attention",
        )(tokens, grad_y, w_q, w_k, w_v, w_o)

        unit_cols = min(256, dim // 2)
        halves = (2, n_slots, TILE, width)
        room = VMEM_LIMIT - math.prod(halves) * 4 - 4 * n_rows * dim - (1 << 20)
        results = pl.pallas_call(
            functools.partial(gather_kernel, n_seq),
            out_shape=(pltpu.VMEM((2, n_rows, dim), BF16), pltpu.VMEM(halves, F32)),
            in_specs=[any_spec] * 6,
            out_specs=(vmem_spec,) * 2,
            scratch_shapes=[pltpu.VMEM((4, n_rows, dim), BF16), pltpu.VMEM((2, dim, unit_cols), BF16), pltpu.VMEM((2, 3, unit_cols, dim), BF16)]
            + [dma((1 + pieces,)), dma((2, 4)), dma((n_chips - 1, pieces)), dma((n_chips - 1, pieces)), dma((2, n_chips, pieces))],
            compiler_params=params(1, room),
            name="gather",
        )(red, own, w_q, w_k, w_v, w_o)

        return pl.pallas_call(
            place_kernel,
            out_shape=(jax.ShapeDtypeStruct((n_rows, dim), BF16),) * 2 + (jax.ShapeDtypeStruct((dim, dim), F32),) * 4,
            in_specs=[vmem_spec] * 2,
            out_specs=(any_spec,) * 6,
            scratch_shapes=[dma((4,))],
            compiler_params=pltpu.CompilerParams(vmem_limit_bytes=1 << 20),
            name="place",
        )(*results)

    return jax.shard_map(local_layer, mesh=mesh, in_specs=(row_spec, P(), P(), P(), P(), row_spec), out_specs=(row_spec, row_spec, grad_spec, grad_spec, grad_spec, grad_spec), check_vma=False)
```

```python
import functools
import math
import jax
import jax.numpy as jnp
from jax import lax
from jax.experimental import pallas as pl
from jax.experimental.pallas import tpu as pltpu
from jax.sharding import PartitionSpec as P

HEAD_DIM = 128
BLOCK_LEN = 128
TILE = 128
ROWS = 256
PARTS = 2
MESH = pl.DeviceIdType.MESH
VMEM_LIMIT = 67_043_328
F32 = jnp.float32
BF16 = jnp.bfloat16


def dot_t(lhs, rhs):
    return lax.dot_general(lhs, rhs, (((0,), (0,)), ((), ())), preferred_element_type=F32)


def dot_nt(lhs, rhs):
    return lax.dot_general(lhs, rhs, (((1,), (1,)), ((), ())), preferred_element_type=F32)


def dot(lhs, rhs):
    return jnp.dot(lhs, rhs, preferred_element_type=F32)


def aligned(index, size):
    return pl.ds(pl.multiple_of(index * size, size), size)


def position(n_seq):
    me = lax.axis_index("sp")
    core, chip = lax.rem(me, 2), lax.div(me, 2)
    return core, chip, n_seq // 2, me + 1 - 2 * core


def send(src, dst, send_sem, recv_sem, target):
    return pltpu.make_async_remote_copy(src_ref=src, dst_ref=dst, send_sem=send_sem, recv_sem=recv_sem, device_id={"sp": target}, device_id_type=MESH)


def entry_barrier(targets):
    barrier = pltpu.get_barrier_semaphore()
    for target in targets:
        pl.semaphore_signal(barrier, inc=1, device_id={"sp": target}, device_id_type=MESH)
    pl.semaphore_wait(barrier, len(targets))


def ring(n_seq):
    core, chip, n_chips, peer = position(n_seq)
    me = lax.axis_index("sp")
    rank = (1 - core) * chip + core * lax.rem(n_chips - chip, n_chips)
    following = lax.rem(me + 2 - 4 * core + n_seq, n_seq)
    previous = lax.rem(me - 2 + 4 * core + n_seq, n_seq)
    return core, rank, n_chips, peer, following, previous


def attention_kernel(n_seq, scale, x, dy, wq, wk, wv, wo, red_out, own_out, xo, ra, w_s, q, do, grads, land, s_in, s_out, r_in, r_out, x_sems, w_sems, chain_sems, send_sems, recv_sems, own_sems, red_sems, credits):
    _, chip, _, _ = position(n_seq)
    core, rank, n_chips, peer, following, previous = ring(n_seq)
    me = lax.axis_index("sp")
    up, down = lax.rem(me + 2, n_seq), lax.rem(me + n_seq - 2, n_seq)
    n_rows, dim = x.shape
    all_rows, width = q.shape
    n_heads = width // HEAD_DIM
    n_blocks = all_rows // BLOCK_LEN
    n_slots = grads.shape[0]
    per_weight = dim // TILE
    early = 2 * per_weight // n_chips
    own_rows, peer_rows = aligned(core, n_rows), aligned(1 - core, n_rows)
    w_cols = aligned(core, width)
    k_col, v_col, a_row, b_row = width + dim, 2 * width + dim, 0, all_rows
    kv_slot, qdo_slot = 0, n_slots // 2

    entry_barrier((peer, up, down))
    x_part, dy_part = pl.ds(0, dim), pl.ds(width, dim)
    local, remote = [], []
    for index, (src, dst) in enumerate(((x, xo.at[own_rows, x_part]), (dy, ra.at[own_rows, dy_part]))):
        remote.append(send(src, dst, x_sems.at[index, 0], x_sems.at[index, 1], peer))
        local.append(pltpu.make_async_copy(src, dst, x_sems.at[index, 2]))
    w_loads = [pltpu.make_async_copy(weight.at[:, w_cols], w_s.at[pl.ds(index * dim, dim)], w_sems.at[index]) for index, weight in enumerate((wk, wv, wq))]
    for part in range(2):
        w_loads.append(pltpu.make_async_copy(wo.at[w_cols, pl.ds(part * width, width)], w_s.at[pl.ds(3 * dim + part * width, width)], w_sems.at[3 + part]))
    remote[0].start()
    local[0].start()
    for load in w_loads[:2]:
        load.start()
    remote[1].start()
    for load in w_loads[2:]:
        load.start()
    local[1].start()

    def weight(index, size):
        return w_s[pl.ds(index * size, size), :]

    def part_rows(half, step):
        return pl.ds(pl.multiple_of(half * n_rows + step * ROWS, ROWS), ROWS)

    def project_kv(half):
        @pl.loop(0, n_rows // ROWS)
        def _(step):
            rows = part_rows(half, step)
            ra[rows, pl.ds(k_col, width)] = dot(xo[rows, x_part], weight(0, dim)).astype(BF16)
            ra[rows, pl.ds(v_col, width)] = dot(xo[rows, x_part], weight(1, dim)).astype(BF16)

    local[0].wait()
    w_loads[0].wait()
    w_loads[1].wait()
    project_kv(core)
    remote[0].wait()
    project_kv(1 - core)

    def head(h, column=0):
        start = column + h * HEAD_DIM
        return pl.ds(start if isinstance(h, int) else pl.multiple_of(start, HEAD_DIM), HEAD_DIM)

    def state_of(ref, h):
        return ref[pl.ds(h * PARTS, PARTS)].reshape(HEAD_DIM, HEAD_DIM)

    def accumulate(left, right, slot, total, reverse):
        total[...] = jnp.zeros_like(total)

        @pl.loop(0, n_blocks)
        def _(step):
            block = (n_blocks - 1 - step) if reverse else step
            rows = aligned(block, BLOCK_LEN)
            for h in range(n_heads):
                running = state_of(total, h)
                grads[slot + block, :, head(h)] = running
                total[pl.ds(h * PARTS, PARTS)] = (running + dot_t(left(rows, h), right(rows, h))).reshape(PARTS, HEAD_DIM // PARTS, HEAD_DIM)

    def q_of(rows, h):
        return q[rows, head(h)]

    def do_of(rows, h):
        return do[rows, head(h)]

    def k_of(rows, h):
        return ra[rows, head(h, k_col)]

    def v_of(rows, h):
        return ra[rows, head(h, v_col)]

    def chain_copy(which, unit):
        src, dst, target = ((s_out, s_in, up), (r_out, r_in, down))[which]
        return send(src.at[unit], dst.at[unit], chain_sems.at[which, 0, unit], chain_sems.at[which, 1, unit], target)

    def chain_step(which, h):
        first, last = ((0, n_chips - 1), (n_chips - 1, 0))[which]
        src, dst = ((s_out, s_in), (r_out, r_in))[which]
        for part in range(PARTS):
            unit = h * PARTS + part

            @pl.when(chip == first)
            def _():
                dst[unit] = jnp.zeros_like(dst[unit])

            @pl.when(chip != first)
            def _():
                chain_copy(which, unit).wait_recv()
                src[unit] = src[unit] + dst[unit]

            @pl.when(chip != last)
            def _():
                chain_copy(which, unit).start()

    steps = n_rows // ROWS
    stride = n_blocks // 4
    due, last_tick = lax.div(5 * chip, 2), 2 * steps + 4

    def chain_s(tick):
        @pl.when((tick >= due) & (tick < due + n_heads))
        def _():
            chain_step(0, tick - due)

    accumulate(k_of, v_of, kv_slot, s_out, False)

    def project_qdo(half, first_tick):
        @pl.loop(0, steps)
        def _(step):
            chain_s(first_tick + step)
            rows = part_rows(half, step)
            q[rows, :] = dot(xo[rows, x_part], weight(2, dim)).astype(BF16)
            product = dot_nt(ra[rows, pl.ds(width, width)], weight(6, width))
            product += dot_nt(ra[rows, pl.ds(2 * width, width)], weight(7, width))
            do[rows, :] = product.astype(BF16)

    for load in w_loads[2:] + [local[1]]:
        load.wait()
    project_qdo(core, 0)
    remote[1].wait()
    project_qdo(1 - core, steps)

    causal = lax.broadcasted_iota(jnp.int32, (BLOCK_LEN, BLOCK_LEN), 0) >= lax.broadcasted_iota(jnp.int32, (BLOCK_LEN, BLOCK_LEN), 1)

    def block_scores(block):
        rows = aligned(block, BLOCK_LEN)
        a_rows = pl.ds(pl.multiple_of(a_row + block * BLOCK_LEN, BLOCK_LEN), BLOCK_LEN)
        b_rows = pl.ds(pl.multiple_of(b_row + block * BLOCK_LEN, BLOCK_LEN), BLOCK_LEN)
        for h in range(n_heads):
            w_s[a_rows, head(h)] = jnp.where(causal, dot_nt(q_of(rows, h), k_of(rows, h)), 0.0).astype(BF16)
            w_s[b_rows, head(h)] = jnp.where(causal, dot_nt(do_of(rows, h), v_of(rows, h)), 0.0).astype(BF16)

    @pl.loop(0, n_blocks)
    def _(block):
        @pl.when(lax.rem(block, stride) == 0)
        def _():
            chain_s(2 * steps + lax.div(block, stride))

        block_scores(block)

    def scores(block, h):
        a_rows = pl.ds(pl.multiple_of(a_row + block * BLOCK_LEN, BLOCK_LEN), BLOCK_LEN)
        b_rows = pl.ds(pl.multiple_of(b_row + block * BLOCK_LEN, BLOCK_LEN), BLOCK_LEN)
        return w_s[a_rows, head(h)], w_s[b_rows, head(h)]

    def both(left, right, top, bottom):
        out = dot(jnp.concatenate([left, right], axis=1), jnp.concatenate([top, bottom], axis=0))
        return (out * scale).astype(BF16)

    group = 4

    @pl.loop(0, n_heads)
    def _(h):
        @pl.when(due + h >= last_tick)
        def _():
            chain_step(0, h)

        incoming = state_of(s_in, h)

        @pl.loop(0, n_blocks // group)
        def _(part):
            for inner in range(group):
                block = part * group + inner
                rows = aligned(block, BLOCK_LEN)
                a, b = scores(block, h)
                s = (incoming + grads[kv_slot + block, :, head(h)]).astype(BF16)
                xo[rows, head(h, dim)] = both(a, q_of(rows, h), v_of(rows, h), s)
                ra[rows, head(h)] = both(b, do_of(rows, h), k_of(rows, h), s.T)

    def rev_head(h):
        incoming = state_of(r_in, h)

        @pl.loop(0, n_blocks // group)
        def _(part):
            for inner in range(group):
                block = part * group + inner
                rows = aligned(block, BLOCK_LEN)
                a, b = scores(block, h)
                r = (incoming + grads[qdo_slot + block, :, head(h)]).astype(BF16)
                dk = both(b.T, v_of(rows, h), q_of(rows, h), r.T)
                dv = both(a.T, k_of(rows, h), do_of(rows, h), r)
                ra[rows, head(h, k_col)] = dk
                ra[rows, head(h, v_col)] = dv

    def credit(which):
        pl.semaphore_signal(credits.at[which], inc=1, device_id={"sp": previous}, device_id_type=MESH)

    def term(late, unit):
        inside, second = lax.rem(unit, per_weight), lax.div(unit, per_weight)
        if late:
            left, right = inside, 3 + second
        else:
            left = (1 - second) * inside + second * (per_weight + lax.div(inside, 2))
            right = second * (1 + lax.rem(inside, 2))
        return dot_t(xo[:, aligned(left, TILE)], ra[:, aligned(right, width)])

    def unit_of(step, piece):
        return lax.rem(rank - step + n_chips, n_chips) * early + piece

    def hop(late, step, piece):
        slot = grads.at[late * (n_slots // 2) + unit_of(step, piece)]
        sems = send_sems.at[late, step, piece], recv_sems.at[late, step, piece]
        return slot, sems

    def start_hop(late, step, piece, first):
        slot, sems = hop(late, step, piece)
        send(slot, land.at[late * early + piece] if first else slot, *sems, following).start()

    def run_ring(late, extra):
        offset = late * (n_slots // 2)

        @pl.loop(0, early)
        def _(piece):
            unit = unit_of(0, piece)
            grads[offset + unit] = term(late, unit)
            start_hop(late, 0, piece, True)

        @pl.loop(0, (n_chips - 1) * early)
        def _(index):
            step, piece = lax.div(index, early) + 1, lax.rem(index, early)
            unit = unit_of(step, piece)
            slot = offset + unit
            extra(index)
            mine = term(late, unit)

            @pl.when(step == 1)
            def _():
                place = land.at[late * early + piece]
                send(place, place, send_sems.at[late, 0, piece], recv_sems.at[late, 0, piece], following).wait_recv()
                grads[slot] = place[...] + mine

            @pl.when(step > 1)
            def _():
                place = grads.at[slot]
                send(place, place, send_sems.at[late, step - 1, piece], recv_sems.at[late, step - 1, piece], following).wait_recv()
                grads[slot] = grads[slot] + mine

            @pl.when(index == 0)
            def _():
                pl.semaphore_wait(credits.at[late], 1)

            @pl.when(step < n_chips - 1)
            def _():
                start_hop(late, step, piece, False)

            @pl.when(step == n_chips - 1)
            def _():
                pltpu.make_async_copy(grads.at[slot], red_out.at[late * early + piece], red_sems.at[late * early + piece]).start()

    gap = ((n_chips - 1) * early - n_heads) // (n_chips - 1)
    rev_start = gap * (n_chips - 1 - chip)

    def reverse_work(index):
        @pl.when(index == 0)
        def _():
            accumulate(q_of, do_of, qdo_slot, r_out, True)

        @pl.when((index >= rev_start) & (index < rev_start + n_heads))
        def _():
            chain_step(1, index - rev_start)
            rev_head(index - rev_start)

        @pl.when(index == rev_start + n_heads - 1)
        def _():
            credit(1)

    credit(0)
    run_ring(0, reverse_work)

    copies = []
    for index, (src, column) in enumerate(((xo, dim), (ra, 0), (ra, k_col), (ra, v_col))):
        part = pl.ds(column, width)
        copies.append(pltpu.make_async_copy(src.at[own_rows, part], own_out.at[index, :, w_cols], own_sems.at[index, 0]))
        copies.append(send(src.at[peer_rows, part], own_out.at[index, :, w_cols], own_sems.at[index, 1], own_sems.at[index, 2], peer))
    for copy in copies:
        copy.start()

    run_ring(1, lambda index: None)

    for which, last in ((0, n_chips - 1), (1, 0)):
        @pl.when(chip != last)
        def _():
            for unit in range(n_heads * PARTS):
                chain_copy(which, unit).wait_send()

    for late in range(2):
        @pl.loop(0, (n_chips - 1) * early)
        def _(index):
            step, piece = lax.div(index, early), lax.rem(index, early)
            slot, sems = hop(late, step, piece)
            send(slot, slot, *sems, following).wait_send()

    for copy in copies:
        copy.wait()
    for late in range(2):
        for piece in range(early):
            slot = late * (n_slots // 2) + lax.rem(rank + 1, n_chips) * early + piece
            pltpu.make_async_copy(grads.at[slot], red_out.at[late * early + piece], red_sems.at[late * early + piece]).wait()


def tile_slot(chunk, piece, early):
    return chunk * early + lax.rem(piece, early), lax.div(piece, early)


def gather_kernel(n_seq, red, own, wq, wk, wv, wo, rows_out, both_out, own_s, wo_s, w_s, own_sems, w_sems, send_sems, recv_sems, peer_sems):
    core, rank, n_chips, peer, following, previous = ring(n_seq)
    mine_out, peer_out = both_out.at[0], both_out.at[1]
    y_out, dx_out = rows_out.at[0], rows_out.at[1]
    n_slots, _, width = mine_out.shape
    dim = 2 * width
    early = 2 * (dim // TILE) // n_chips
    pieces = 2 * early
    n_rows = own.shape[1]
    unit_cols = wo_s.shape[2]
    n_units = dim // unit_cols
    row_blocks = n_rows // ROWS

    def slot_of(chunk, piece):
        unit, late = tile_slot(chunk, piece, early)
        return unit + late * (n_slots // 2)

    def held(step, piece):
        return slot_of(lax.rem(rank + 1 - step + n_chips, n_chips), piece)

    def w_loads(unit, buffer):
        part = aligned(unit, unit_cols)
        loads = [pltpu.make_async_copy(wo.at[:, part], wo_s.at[buffer], w_sems.at[buffer, 0])]
        for index, weight in enumerate((wq, wk, wv)):
            loads.append(pltpu.make_async_copy(weight.at[part], w_s.at[buffer, index], w_sems.at[buffer, 1 + index]))
        return loads

    own_load = pltpu.make_async_copy(own, own_s, own_sems.at[0])
    own_load.start()
    for unit in range(2):
        for load in w_loads(unit, unit):
            load.start()
    red_loads = [pltpu.make_async_copy(red.at[piece], mine_out.at[held(0, piece)], own_sems.at[1 + piece]) for piece in range(pieces)]
    for load in red_loads:
        load.start()

    entry_barrier((peer, following, previous))

    def to_next(step, piece):
        slot = held(step, piece)
        return send(mine_out.at[slot], mine_out.at[slot], send_sems.at[step, piece], recv_sems.at[step, piece], following)

    def arrival(step, piece):
        slot = held(step + 1, piece)
        return send(mine_out.at[slot], mine_out.at[slot], send_sems.at[step, piece], recv_sems.at[step, piece], following)

    def to_peer(step, piece):
        slot = held(step, piece)
        return send(mine_out.at[slot], peer_out.at[slot], peer_sems.at[0, step, piece], peer_sems.at[1, step, piece], peer)

    for piece in range(pieces):
        red_loads[piece].wait()
        to_next(0, piece).start()
        to_peer(0, piece).start()
    own_load.wait()

    def project(unit, block):
        buffer = lax.rem(unit, 2)

        @pl.when(block == 0)
        def _():
            for load in w_loads(unit, buffer):
                load.wait()

        rows, cols = aligned(block, ROWS), aligned(unit, unit_cols)
        y_out[rows, cols] = dot(own_s[0, rows, :], wo_s[buffer]).astype(BF16)
        total = dot_nt(own_s[1, rows, :], w_s[buffer, 0])
        total += dot_nt(own_s[2, rows, :], w_s[buffer, 1])
        total += dot_nt(own_s[3, rows, :], w_s[buffer, 2])
        dx_out[rows, cols] = total.astype(BF16)

        @pl.when((block == row_blocks - 1) & (unit + 2 < n_units))
        def _():
            for load in w_loads(unit + 2, buffer):
                load.start()

    @pl.loop(0, (n_chips - 1) * pieces)
    def _(index):
        step, piece = lax.div(index, pieces), lax.rem(index, pieces)

        @pl.when(index < n_units * row_blocks)
        def _():
            project(lax.div(index, row_blocks), lax.rem(index, row_blocks))

        arrival(step, piece).wait_recv()

        @pl.when(step < n_chips - 2)
        def _():
            to_next(step + 1, piece).start()

        to_peer(step + 1, piece).start()

    @pl.loop(0, n_chips * pieces)
    def _(index):
        step, piece = lax.div(index, pieces), lax.rem(index, pieces)

        @pl.when(step < n_chips - 1)
        def _():
            to_next(step, piece).wait_send()

        to_peer(step, piece).wait()


def place_kernel(results, both, y, dx, gq, gk, gv, go, sems):
    core = lax.rem(lax.axis_index("sp"), 2)
    _, n_slots, _, width = both.shape
    per_weight = n_slots // 4
    copies = [pltpu.make_async_copy(results.at[0], y, sems.at[2]), pltpu.make_async_copy(results.at[1], dx, sems.at[3])]
    for side, half in enumerate((core, 1 - core)):
        cols = aligned(half, width)
        for slot in range(n_slots):
            weight, inside = slot // per_weight, slot % per_weight
            if weight == 1:
                rows = pl.ds(pl.multiple_of(half * width + inside // 2 * TILE, TILE), TILE)
                dst = go.at[rows, pl.ds(inside % 2 * width, width)]
            else:
                dst = (gq, None, gk, gv)[weight].at[pl.ds(inside * TILE, TILE), cols]
            copies.append(pltpu.make_async_copy(both.at[side, slot], dst, sems.at[side]))
    for copy in copies:
        copy.start()
    for copy in copies:
        copy.wait()


def solution(mesh):
    n_seq = mesh.shape["sp"]
    n_chips = n_seq // 2
    row_spec = P(("dp", "sp"), None)
    grad_spec = P("dp", None)
    any_spec = pl.BlockSpec(memory_space=pl.ANY)
    vmem_spec = pl.BlockSpec(memory_space=pltpu.VMEM)
    dma = pltpu.SemaphoreType.DMA

    def params(collective_id, limit=VMEM_LIMIT):
        return pltpu.CompilerParams(collective_id=collective_id, has_side_effects=True, vmem_limit_bytes=limit)

    def local_layer(tokens, w_q, w_k, w_v, w_o, grad_y):
        n_rows, dim = tokens.shape
        width = dim // 2
        n_heads = width // HEAD_DIM
        rows = 2 * n_rows
        n_slots = 4 * (dim // TILE)
        pieces = n_slots // n_chips
        scale = 1.0 / math.sqrt(n_rows * n_seq * HEAD_DIM)
        state = (n_heads * PARTS, HEAD_DIM // PARTS, HEAD_DIM)

        red, own = pl.pallas_call(
            functools.partial(attention_kernel, n_seq, scale),
            out_shape=(jax.ShapeDtypeStruct((pieces, TILE, width), F32), jax.ShapeDtypeStruct((4, n_rows, dim), BF16)),
            in_specs=[any_spec] * 6,
            out_specs=(any_spec,) * 2,
            scratch_shapes=[pltpu.VMEM((rows, dim + width), BF16), pltpu.VMEM((rows, dim + 3 * width), BF16), pltpu.VMEM((4 * dim, width), BF16)]
            + [pltpu.VMEM((rows, width), BF16)] * 2
            + [pltpu.VMEM((n_slots, TILE, width), F32), pltpu.VMEM((pieces, TILE, width), F32)]
            + [pltpu.VMEM(state, F32)] * 4
            + [dma((2, 3)), dma((5,)), dma((2, 2, n_heads * PARTS))]
            + [dma((2, n_chips - 1, pieces // 2))] * 2
            + [dma((4, 3)), dma((pieces,)), pltpu.SemaphoreType.REGULAR((2,))],
            compiler_params=params(0),
            name="attention",
        )(tokens, grad_y, w_q, w_k, w_v, w_o)

        unit_cols = min(256, dim // 2)
        halves = (2, n_slots, TILE, width)
        room = VMEM_LIMIT - math.prod(halves) * 4 - 4 * n_rows * dim - (1 << 20)
        results = pl.pallas_call(
            functools.partial(gather_kernel, n_seq),
            out_shape=(pltpu.VMEM((2, n_rows, dim), BF16), pltpu.VMEM(halves, F32)),
            in_specs=[any_spec] * 6,
            out_specs=(vmem_spec,) * 2,
            scratch_shapes=[pltpu.VMEM((4, n_rows, dim), BF16), pltpu.VMEM((2, dim, unit_cols), BF16), pltpu.VMEM((2, 3, unit_cols, dim), BF16)]
            + [dma((1 + pieces,)), dma((2, 4)), dma((n_chips - 1, pieces)), dma((n_chips - 1, pieces)), dma((2, n_chips, pieces))],
            compiler_params=params(1, room),
            name="gather",
        )(red, own, w_q, w_k, w_v, w_o)

        return pl.pallas_call(
            place_kernel,
            out_shape=(jax.ShapeDtypeStruct((n_rows, dim), BF16),) * 2 + (jax.ShapeDtypeStruct((dim, dim), F32),) * 4,
            in_specs=[vmem_spec] * 2,
            out_specs=(any_spec,) * 6,
            scratch_shapes=[dma((4,))],
            compiler_params=pltpu.CompilerParams(vmem_limit_bytes=1 << 20),
            name="place",
        )(*results)

    return jax.shard_map(local_layer, mesh=mesh, in_specs=(row_spec, P(), P(), P(), P(), row_spec), out_specs=(row_spec, row_spec, grad_spec, grad_spec, grad_spec, grad_spec), check_vma=False)
```

```python
import functools
import math
import jax
import jax.numpy as jnp
from jax import lax
from jax.experimental import pallas as pl
from jax.experimental.pallas import tpu as pltpu
from jax.sharding import PartitionSpec as P

HEAD_DIM = 128
BLOCK_LEN = 128
TILE = 128
ROWS = 256
PROJECT_ROWS = 512
MESH = pl.DeviceIdType.MESH
VMEM_LIMIT = 67_043_328
F32 = jnp.float32
BF16 = jnp.bfloat16


def dot_t(lhs, rhs):
    return lax.dot_general(lhs, rhs, (((0,), (0,)), ((), ())), preferred_element_type=F32)


def dot_nt(lhs, rhs):
    return lax.dot_general(lhs, rhs, (((1,), (1,)), ((), ())), preferred_element_type=F32)


def dot(lhs, rhs):
    return jnp.dot(lhs, rhs, preferred_element_type=F32)


def aligned(index, size):
    return pl.ds(pl.multiple_of(index * size, size), size)


def position(n_seq):
    me = lax.axis_index("sp")
    core, chip = lax.rem(me, 2), lax.div(me, 2)
    return core, chip, n_seq // 2, me + 1 - 2 * core


def send(src, dst, send_sem, recv_sem, target):
    return pltpu.make_async_remote_copy(src_ref=src, dst_ref=dst, send_sem=send_sem, recv_sem=recv_sem, device_id={"sp": target}, device_id_type=MESH)


def entry_barrier(targets):
    barrier = pltpu.get_barrier_semaphore()
    for target in targets:
        pl.semaphore_signal(barrier, inc=1, device_id={"sp": target}, device_id_type=MESH)
    pl.semaphore_wait(barrier, len(targets))


def ring(n_seq):
    core, chip, n_chips, peer = position(n_seq)
    me = lax.axis_index("sp")
    rank = (1 - core) * chip + core * lax.rem(n_chips - chip, n_chips)
    following = lax.rem(me + 2 - 4 * core + n_seq, n_seq)
    previous = lax.rem(me - 2 + 4 * core + n_seq, n_seq)
    return core, rank, n_chips, peer, following, previous


def attention_kernel(n_seq, scale, x, dy, wq, wk, wv, wo, red_out, own_out, xo, ra, w_s, q, do, grads, land, s_in, s_out, r_in, r_out, x_sems, w_sems, chain_sems, send_sems, recv_sems, own_sems, red_sems, credits):
    _, chip, _, _ = position(n_seq)
    core, rank, n_chips, peer, following, previous = ring(n_seq)
    me = lax.axis_index("sp")
    up, down = lax.rem(me + 2, n_seq), lax.rem(me + n_seq - 2, n_seq)
    n_rows, dim = x.shape
    all_rows, width = q.shape
    n_heads = width // HEAD_DIM
    n_blocks = all_rows // BLOCK_LEN
    n_slots = grads.shape[0]
    per_weight = dim // TILE
    early = 2 * per_weight // n_chips
    own_rows, peer_rows = aligned(core, n_rows), aligned(1 - core, n_rows)
    w_cols = aligned(core, width)
    k_col, v_col, a_row, b_row = width + dim, 2 * width + dim, 0, all_rows
    kv_slot, qdo_slot = 0, n_slots // 2

    entry_barrier((peer, up, down))
    x_part, dy_part = pl.ds(0, dim), pl.ds(width, dim)
    local, remote = [], []
    for index, (src, dst) in enumerate(((x, xo.at[own_rows, x_part]), (dy, ra.at[own_rows, dy_part]))):
        remote.append(send(src, dst, x_sems.at[index, 0], x_sems.at[index, 1], peer))
        local.append(pltpu.make_async_copy(src, dst, x_sems.at[index, 2]))
    w_loads = [pltpu.make_async_copy(weight.at[:, w_cols], w_s.at[pl.ds(index * dim, dim)], w_sems.at[index]) for index, weight in enumerate((wk, wv, wq))]
    for part in range(2):
        w_loads.append(pltpu.make_async_copy(wo.at[w_cols, pl.ds(part * width, width)], w_s.at[pl.ds(3 * dim + part * width, width)], w_sems.at[3 + part]))
    remote[0].start()
    local[0].start()
    for load in w_loads[:2]:
        load.start()
    remote[1].start()
    for load in w_loads[2:]:
        load.start()
    local[1].start()

    def weight(index, size):
        return w_s[pl.ds(index * size, size), :]

    part_len = min(PROJECT_ROWS, n_rows)
    steps = n_rows // part_len

    def part_rows(half, step):
        return pl.ds(pl.multiple_of(half * n_rows + step * part_len, part_len), part_len)

    def project_kv(half):
        @pl.loop(0, steps)
        def _(step):
            rows = part_rows(half, step)
            ra[rows, pl.ds(k_col, width)] = dot(xo[rows, x_part], weight(0, dim)).astype(BF16)
            ra[rows, pl.ds(v_col, width)] = dot(xo[rows, x_part], weight(1, dim)).astype(BF16)

    local[0].wait()
    w_loads[0].wait()
    w_loads[1].wait()
    project_kv(core)
    remote[0].wait()
    project_kv(1 - core)

    def head(h, column=0):
        return pl.ds(column + h * HEAD_DIM, HEAD_DIM)

    def accumulate(left, right, slot, total, reverse):
        total[...] = jnp.zeros_like(total)

        @pl.loop(0, n_blocks // 2)
        def _(step):
            for inner in range(2):
                block = (n_blocks - 1 - 2 * step - inner) if reverse else 2 * step + inner
                rows = aligned(block, BLOCK_LEN)
                for h in range(n_heads):
                    running = total[h]
                    grads[slot + block, :, head(h)] = running
                    total[h] = running + dot_t(left(rows, h), right(rows, h))

    def q_of(rows, h):
        return q[rows, head(h)]

    def do_of(rows, h):
        return do[rows, head(h)]

    def k_of(rows, h):
        return ra[rows, head(h, k_col)]

    def v_of(rows, h):
        return ra[rows, head(h, v_col)]

    def chain_copy(which, h):
        src, dst, target = ((s_out, s_in, up), (r_out, r_in, down))[which]
        return send(src.at[h], dst.at[h], chain_sems.at[which, 0, h], chain_sems.at[which, 1, h], target)

    def chain_step(which, h):
        first, last = ((0, n_chips - 1), (n_chips - 1, 0))[which]
        src, dst = ((s_out, s_in), (r_out, r_in))[which]

        @pl.when(chip == first)
        def _():
            dst[h] = jnp.zeros_like(dst[h])

        @pl.when(chip != first)
        def _():
            chain_copy(which, h).wait_recv()
            src[h] = src[h] + dst[h]

        @pl.when(chip != last)
        def _():
            chain_copy(which, h).start()

    def chain_s(tick):
        @pl.when((tick >= 3 * chip) & (tick < 3 * chip + n_heads))
        def _():
            chain_step(0, tick - 3 * chip)

    accumulate(k_of, v_of, kv_slot, s_out, False)

    def project_qdo(half, first_tick):
        @pl.loop(0, steps)
        def _(step):
            chain_s(first_tick + 2 * step)
            chain_s(first_tick + 2 * step + 1)
            rows = part_rows(half, step)
            q[rows, :] = dot(xo[rows, x_part], weight(2, dim)).astype(BF16)
            product = dot_nt(ra[rows, pl.ds(width, width)], weight(6, width))
            product += dot_nt(ra[rows, pl.ds(2 * width, width)], weight(7, width))
            do[rows, :] = product.astype(BF16)

    for load in w_loads[2:] + [local[1]]:
        load.wait()
    project_qdo(core, 0)
    remote[1].wait()
    project_qdo(1 - core, 2 * steps)

    causal = lax.broadcasted_iota(jnp.int32, (BLOCK_LEN, BLOCK_LEN), 0) >= lax.broadcasted_iota(jnp.int32, (BLOCK_LEN, BLOCK_LEN), 1)

    def block_scores(block):
        rows = aligned(block, BLOCK_LEN)
        a_rows = pl.ds(pl.multiple_of(a_row + block * BLOCK_LEN, BLOCK_LEN), BLOCK_LEN)
        b_rows = pl.ds(pl.multiple_of(b_row + block * BLOCK_LEN, BLOCK_LEN), BLOCK_LEN)
        for h in range(n_heads):
            w_s[a_rows, head(h)] = jnp.where(causal, dot_nt(q_of(rows, h), k_of(rows, h)), 0.0).astype(BF16)
            w_s[b_rows, head(h)] = jnp.where(causal, dot_nt(do_of(rows, h), v_of(rows, h)), 0.0).astype(BF16)

    @pl.loop(0, max(3 * (n_chips - 1) + n_heads - 4 * steps, n_blocks // 2))
    def _(step):
        chain_s(4 * steps + step)

        @pl.when(step < n_blocks // 2)
        def _():
            for inner in range(2):
                block_scores(2 * step + inner)

    def scores(block, h):
        a_rows = pl.ds(pl.multiple_of(a_row + block * BLOCK_LEN, BLOCK_LEN), BLOCK_LEN)
        b_rows = pl.ds(pl.multiple_of(b_row + block * BLOCK_LEN, BLOCK_LEN), BLOCK_LEN)
        return w_s[a_rows, head(h)], w_s[b_rows, head(h)]

    def both(left, right, top, bottom):
        out = dot(jnp.concatenate([left, right], axis=1), jnp.concatenate([top, bottom], axis=0))
        return (out * scale).astype(BF16)

    @pl.loop(0, n_blocks // 2)
    def _(step):
        for inner in range(2):
            block = 2 * step + inner
            rows = aligned(block, BLOCK_LEN)
            for h in range(n_heads):
                a, b = scores(block, h)
                s = (s_in[h] + grads[kv_slot + block, :, head(h)]).astype(BF16)
                xo[rows, head(h, dim)] = both(a, q_of(rows, h), v_of(rows, h), s)
                ra[rows, head(h)] = both(b, do_of(rows, h), k_of(rows, h), s.T)

    def rev_block(block):
        rows = aligned(block, BLOCK_LEN)
        for h in range(n_heads):
            a, b = scores(block, h)
            r = (r_in[h] + grads[qdo_slot + block, :, head(h)]).astype(BF16)
            dk = both(b.T, v_of(rows, h), q_of(rows, h), r.T)
            dv = both(a.T, k_of(rows, h), do_of(rows, h), r)
            ra[rows, head(h, k_col)] = dk
            ra[rows, head(h, v_col)] = dv

    def credit(which):
        pl.semaphore_signal(credits.at[which], inc=1, device_id={"sp": previous}, device_id_type=MESH)

    def term(late, unit):
        inside, second = lax.rem(unit, per_weight), lax.div(unit, per_weight)
        if late:
            left, right = inside, 3 + second
        else:
            left = (1 - second) * inside + second * (per_weight + lax.div(inside, 2))
            right = second * (1 + lax.rem(inside, 2))
        return dot_t(xo[:, aligned(left, TILE)], ra[:, aligned(right, width)])

    def unit_of(step, piece):
        return lax.rem(rank - step + n_chips, n_chips) * early + piece

    def hop(late, step, piece):
        slot = grads.at[late * (n_slots // 2) + unit_of(step, piece)]
        sems = send_sems.at[late, step, piece], recv_sems.at[late, step, piece]
        return slot, sems

    def start_hop(late, step, piece, first):
        slot, sems = hop(late, step, piece)
        send(slot, land.at[late * early + piece] if first else slot, *sems, following).start()

    def run_ring(late, extra):
        offset = late * (n_slots // 2)

        @pl.loop(0, early)
        def _(piece):
            unit = unit_of(0, piece)
            grads[offset + unit] = term(late, unit)
            start_hop(late, 0, piece, True)

        @pl.loop(0, (n_chips - 1) * early)
        def _(index):
            step, piece = lax.div(index, early) + 1, lax.rem(index, early)
            unit = unit_of(step, piece)
            slot = offset + unit
            extra(index)
            mine = term(late, unit)

            @pl.when(step == 1)
            def _():
                place = land.at[late * early + piece]
                send(place, place, send_sems.at[late, 0, piece], recv_sems.at[late, 0, piece], following).wait_recv()
                grads[slot] = place[...] + mine

            @pl.when(step > 1)
            def _():
                place = grads.at[slot]
                send(place, place, send_sems.at[late, step - 1, piece], recv_sems.at[late, step - 1, piece], following).wait_recv()
                grads[slot] = grads[slot] + mine

            @pl.when(index == 0)
            def _():
                pl.semaphore_wait(credits.at[late], 1)

            @pl.when(step < n_chips - 1)
            def _():
                start_hop(late, step, piece, False)

            @pl.when(step == n_chips - 1)
            def _():
                pltpu.make_async_copy(grads.at[slot], red_out.at[late * early + piece], red_sems.at[late * early + piece]).start()

    share = n_blocks // 4

    def reverse_work(index):
        @pl.when(index == 0)
        def _():
            accumulate(q_of, do_of, qdo_slot, r_out, True)

        @pl.when(index == n_chips - chip)
        def _():
            for h in range(n_heads):
                chain_step(1, h)

        @pl.when((index > n_chips) & (index <= n_chips + 4))
        def _():
            @pl.loop(0, share)
            def _(part):
                rev_block((index - n_chips - 1) * share + part)

        @pl.when(index == n_chips + 4)
        def _():
            credit(1)

    credit(0)
    run_ring(0, reverse_work)

    copies = []
    for index, (src, column) in enumerate(((xo, dim), (ra, 0), (ra, k_col), (ra, v_col))):
        part = pl.ds(column, width)
        copies.append(pltpu.make_async_copy(src.at[own_rows, part], own_out.at[index, :, w_cols], own_sems.at[index, 0]))
        copies.append(send(src.at[peer_rows, part], own_out.at[index, :, w_cols], own_sems.at[index, 1], own_sems.at[index, 2], peer))
    for copy in copies:
        copy.start()

    run_ring(1, lambda index: None)

    for which, last in ((0, n_chips - 1), (1, 0)):
        @pl.when(chip != last)
        def _():
            for h in range(n_heads):
                chain_copy(which, h).wait_send()

    for late in range(2):
        @pl.loop(0, (n_chips - 1) * early)
        def _(index):
            step, piece = lax.div(index, early), lax.rem(index, early)
            slot, sems = hop(late, step, piece)
            send(slot, slot, *sems, following).wait_send()

    for copy in copies:
        copy.wait()
    for late in range(2):
        for piece in range(early):
            slot = late * (n_slots // 2) + lax.rem(rank + 1, n_chips) * early + piece
            pltpu.make_async_copy(grads.at[slot], red_out.at[late * early + piece], red_sems.at[late * early + piece]).wait()


def tile_slot(chunk, piece, early):
    return chunk * early + lax.rem(piece, early), lax.div(piece, early)


def gather_kernel(n_seq, red, own, wq, wk, wv, wo, rows_out, both_out, own_s, wo_s, w_s, own_sems, w_sems, send_sems, recv_sems, peer_sems):
    core, rank, n_chips, peer, following, previous = ring(n_seq)
    mine_out, peer_out = both_out.at[0], both_out.at[1]
    y_out, dx_out = rows_out.at[0], rows_out.at[1]
    n_slots, _, width = mine_out.shape
    dim = 2 * width
    early = 2 * (dim // TILE) // n_chips
    pieces = 2 * early
    n_rows = own.shape[1]
    unit_cols = wo_s.shape[2]
    n_units = dim // unit_cols
    row_blocks = n_rows // ROWS

    def slot_of(chunk, piece):
        unit, late = tile_slot(chunk, piece, early)
        return unit + late * (n_slots // 2)

    def held(step, piece):
        return slot_of(lax.rem(rank + 1 - step + n_chips, n_chips), piece)

    def w_loads(unit, buffer):
        part = aligned(unit, unit_cols)
        loads = [pltpu.make_async_copy(wo.at[:, part], wo_s.at[buffer], w_sems.at[buffer, 0])]
        for index, weight in enumerate((wq, wk, wv)):
            loads.append(pltpu.make_async_copy(weight.at[part], w_s.at[buffer, index], w_sems.at[buffer, 1 + index]))
        return loads

    own_load = pltpu.make_async_copy(own, own_s, own_sems.at[0])
    own_load.start()
    for unit in range(2):
        for load in w_loads(unit, unit):
            load.start()
    red_loads = [pltpu.make_async_copy(red.at[piece], mine_out.at[held(0, piece)], own_sems.at[1 + piece]) for piece in range(pieces)]
    for load in red_loads:
        load.start()

    entry_barrier((peer, following, previous))

    def to_next(step, piece):
        slot = held(step, piece)
        return send(mine_out.at[slot], mine_out.at[slot], send_sems.at[step, piece], recv_sems.at[step, piece], following)

    def arrival(step, piece):
        slot = held(step + 1, piece)
        return send(mine_out.at[slot], mine_out.at[slot], send_sems.at[step, piece], recv_sems.at[step, piece], following)

    def to_peer(step, piece):
        slot = held(step, piece)
        return send(mine_out.at[slot], peer_out.at[slot], peer_sems.at[0, step, piece], peer_sems.at[1, step, piece], peer)

    for piece in range(pieces):
        red_loads[piece].wait()
        to_next(0, piece).start()
        to_peer(0, piece).start()
    own_load.wait()

    def project(unit, block):
        buffer = lax.rem(unit, 2)

        @pl.when(block == 0)
        def _():
            for load in w_loads(unit, buffer):
                load.wait()

        rows, cols = aligned(block, ROWS), aligned(unit, unit_cols)
        y_out[rows, cols] = dot(own_s[0, rows, :], wo_s[buffer]).astype(BF16)
        total = dot_nt(own_s[1, rows, :], w_s[buffer, 0])
        total += dot_nt(own_s[2, rows, :], w_s[buffer, 1])
        total += dot_nt(own_s[3, rows, :], w_s[buffer, 2])
        dx_out[rows, cols] = total.astype(BF16)

        @pl.when((block == row_blocks - 1) & (unit + 2 < n_units))
        def _():
            for load in w_loads(unit + 2, buffer):
                load.start()

    @pl.loop(0, (n_chips - 1) * pieces)
    def _(index):
        step, piece = lax.div(index, pieces), lax.rem(index, pieces)

        @pl.when(index < n_units * row_blocks)
        def _():
            project(lax.div(index, row_blocks), lax.rem(index, row_blocks))

        arrival(step, piece).wait_recv()

        @pl.when(step < n_chips - 2)
        def _():
            to_next(step + 1, piece).start()

        to_peer(step + 1, piece).start()

    @pl.loop(0, n_chips * pieces)
    def _(index):
        step, piece = lax.div(index, pieces), lax.rem(index, pieces)

        @pl.when(step < n_chips - 1)
        def _():
            to_next(step, piece).wait_send()

        to_peer(step, piece).wait()


def place_kernel(results, both, y, dx, gq, gk, gv, go, sems):
    core = lax.rem(lax.axis_index("sp"), 2)
    _, n_slots, _, width = both.shape
    per_weight = n_slots // 4
    copies = [pltpu.make_async_copy(results.at[0], y, sems.at[2]), pltpu.make_async_copy(results.at[1], dx, sems.at[3])]
    for side, half in enumerate((core, 1 - core)):
        cols = aligned(half, width)
        for slot in range(n_slots):
            weight, inside = slot // per_weight, slot % per_weight
            if weight == 1:
                rows = pl.ds(pl.multiple_of(half * width + inside // 2 * TILE, TILE), TILE)
                dst = go.at[rows, pl.ds(inside % 2 * width, width)]
            else:
                dst = (gq, None, gk, gv)[weight].at[pl.ds(inside * TILE, TILE), cols]
            copies.append(pltpu.make_async_copy(both.at[side, slot], dst, sems.at[side]))
    for copy in copies:
        copy.start()
    for copy in copies:
        copy.wait()


def solution(mesh):
    n_seq = mesh.shape["sp"]
    n_chips = n_seq // 2
    row_spec = P(("dp", "sp"), None)
    grad_spec = P("dp", None)
    any_spec = pl.BlockSpec(memory_space=pl.ANY)
    vmem_spec = pl.BlockSpec(memory_space=pltpu.VMEM)
    dma = pltpu.SemaphoreType.DMA

    def params(collective_id, limit=VMEM_LIMIT):
        return pltpu.CompilerParams(collective_id=collective_id, has_side_effects=True, vmem_limit_bytes=limit)

    def local_layer(tokens, w_q, w_k, w_v, w_o, grad_y):
        n_rows, dim = tokens.shape
        width = dim // 2
        n_heads = width // HEAD_DIM
        rows = 2 * n_rows
        n_slots = 4 * (dim // TILE)
        pieces = n_slots // n_chips
        scale = 1.0 / math.sqrt(n_rows * n_seq * HEAD_DIM)
        state = (n_heads, HEAD_DIM, HEAD_DIM)

        red, own = pl.pallas_call(
            functools.partial(attention_kernel, n_seq, scale),
            out_shape=(jax.ShapeDtypeStruct((pieces, TILE, width), F32), jax.ShapeDtypeStruct((4, n_rows, dim), BF16)),
            in_specs=[any_spec] * 6,
            out_specs=(any_spec,) * 2,
            scratch_shapes=[pltpu.VMEM((rows, dim + width), BF16), pltpu.VMEM((rows, dim + 3 * width), BF16), pltpu.VMEM((4 * dim, width), BF16)]
            + [pltpu.VMEM((rows, width), BF16)] * 2
            + [pltpu.VMEM((n_slots, TILE, width), F32), pltpu.VMEM((pieces, TILE, width), F32)]
            + [pltpu.VMEM(state, F32)] * 4
            + [dma((2, 3)), dma((5,)), dma((2, 2, n_heads))]
            + [dma((2, n_chips - 1, pieces // 2))] * 2
            + [dma((4, 3)), dma((pieces,)), pltpu.SemaphoreType.REGULAR((2,))],
            compiler_params=params(0),
            name="attention",
        )(tokens, grad_y, w_q, w_k, w_v, w_o)

        unit_cols = min(256, dim // 2)
        halves = (2, n_slots, TILE, width)
        room = VMEM_LIMIT - math.prod(halves) * 4 - 4 * n_rows * dim - (1 << 20)
        results = pl.pallas_call(
            functools.partial(gather_kernel, n_seq),
            out_shape=(pltpu.VMEM((2, n_rows, dim), BF16), pltpu.VMEM(halves, F32)),
            in_specs=[any_spec] * 6,
            out_specs=(vmem_spec,) * 2,
            scratch_shapes=[pltpu.VMEM((4, n_rows, dim), BF16), pltpu.VMEM((2, dim, unit_cols), BF16), pltpu.VMEM((2, 3, unit_cols, dim), BF16)]
            + [dma((1 + pieces,)), dma((2, 4)), dma((n_chips - 1, pieces)), dma((n_chips - 1, pieces)), dma((2, n_chips, pieces))],
            compiler_params=params(1, room),
            name="gather",
        )(red, own, w_q, w_k, w_v, w_o)

        return pl.pallas_call(
            place_kernel,
            out_shape=(jax.ShapeDtypeStruct((n_rows, dim), BF16),) * 2 + (jax.ShapeDtypeStruct((dim, dim), F32),) * 4,
            in_specs=[vmem_spec] * 2,
            out_specs=(any_spec,) * 6,
            scratch_shapes=[dma((4,))],
            compiler_params=pltpu.CompilerParams(vmem_limit_bytes=1 << 20),
            name="place",
        )(*results)

    return jax.shard_map(local_layer, mesh=mesh, in_specs=(row_spec, P(), P(), P(), P(), row_spec), out_specs=(row_spec, row_spec, grad_spec, grad_spec, grad_spec, grad_spec), check_vma=False)
```

```python
import functools
import math
import jax
import jax.numpy as jnp
from jax import lax
from jax.experimental import pallas as pl
from jax.experimental.pallas import tpu as pltpu
from jax.sharding import PartitionSpec as P

HEAD_DIM = 128
BLOCK_LEN = 128
TILE = 128
ROWS = 256
PROJECT_ROWS = 512
MESH = pl.DeviceIdType.MESH
VMEM_LIMIT = 67_043_328
F32 = jnp.float32
BF16 = jnp.bfloat16


def dot_t(lhs, rhs):
    return lax.dot_general(lhs, rhs, (((0,), (0,)), ((), ())), preferred_element_type=F32)


def dot_nt(lhs, rhs):
    return lax.dot_general(lhs, rhs, (((1,), (1,)), ((), ())), preferred_element_type=F32)


def dot(lhs, rhs):
    return jnp.dot(lhs, rhs, preferred_element_type=F32)


def aligned(index, size):
    return pl.ds(pl.multiple_of(index * size, size), size)


def position(n_seq):
    me = lax.axis_index("sp")
    core, chip = lax.rem(me, 2), lax.div(me, 2)
    return core, chip, n_seq // 2, me + 1 - 2 * core


def send(src, dst, send_sem, recv_sem, target):
    return pltpu.make_async_remote_copy(src_ref=src, dst_ref=dst, send_sem=send_sem, recv_sem=recv_sem, device_id={"sp": target}, device_id_type=MESH)


def entry_barrier(targets):
    barrier = pltpu.get_barrier_semaphore()
    for target in targets:
        pl.semaphore_signal(barrier, inc=1, device_id={"sp": target}, device_id_type=MESH)
    pl.semaphore_wait(barrier, len(targets))


def ring(n_seq):
    core, chip, n_chips, peer = position(n_seq)
    me = lax.axis_index("sp")
    rank = (1 - core) * chip + core * lax.rem(n_chips - chip, n_chips)
    following = lax.rem(me + 2 - 4 * core + n_seq, n_seq)
    previous = lax.rem(me - 2 + 4 * core + n_seq, n_seq)
    return core, rank, n_chips, peer, following, previous


def attention_kernel(n_seq, scale, x, dy, wq, wk, wv, wo, red_out, own_out, xo, ra, w_s, q, do, grads, land, s_in, s_out, r_in, r_out, x_sems, w_sems, chain_sems, send_sems, recv_sems, own_sems, red_sems, credits):
    _, chip, _, _ = position(n_seq)
    core, rank, n_chips, peer, following, previous = ring(n_seq)
    me = lax.axis_index("sp")
    up, down = lax.rem(me + 2, n_seq), lax.rem(me + n_seq - 2, n_seq)
    n_rows, dim = x.shape
    all_rows, width = q.shape
    n_heads = width // HEAD_DIM
    n_blocks = all_rows // BLOCK_LEN
    n_slots = grads.shape[0]
    per_weight = dim // TILE
    early = 2 * per_weight // n_chips
    own_rows, peer_rows = aligned(core, n_rows), aligned(1 - core, n_rows)
    w_cols = aligned(core, width)
    k_col, v_col, a_row, b_row = width + dim, 2 * width + dim, 0, all_rows
    kv_slot, qdo_slot = 0, n_slots // 2

    x_part, dy_part = pl.ds(0, dim), pl.ds(width, dim)
    local, remote = [], []
    for index, (src, dst) in enumerate(((x, xo.at[own_rows, x_part]), (dy, ra.at[own_rows, dy_part]))):
        local.append(pltpu.make_async_copy(src, dst, x_sems.at[index, 2]))
        remote.append(send(dst, dst, x_sems.at[index, 0], x_sems.at[index, 1], peer))
    w_loads = [pltpu.make_async_copy(weight.at[:, w_cols], w_s.at[pl.ds(index * dim, dim)], w_sems.at[index]) for index, weight in enumerate((wk, wv, wq))]
    for part in range(2):
        w_loads.append(pltpu.make_async_copy(wo.at[w_cols, pl.ds(part * width, width)], w_s.at[pl.ds(3 * dim + part * width, width)], w_sems.at[3 + part]))
    local[0].start()
    for load in w_loads[:2]:
        load.start()
    local[1].start()
    for load in w_loads[2:]:
        load.start()
    entry_barrier((peer, up, down))
    for index in range(2):
        local[index].wait()
        remote[index].start()

    def weight(index, size):
        return w_s[pl.ds(index * size, size), :]

    part_len = min(PROJECT_ROWS, n_rows)
    steps = n_rows // part_len

    def part_rows(half, step):
        return pl.ds(pl.multiple_of(half * n_rows + step * part_len, part_len), part_len)

    def project_kv(half):
        @pl.loop(0, steps)
        def _(step):
            rows = part_rows(half, step)
            ra[rows, pl.ds(k_col, width)] = dot(xo[rows, x_part], weight(0, dim)).astype(BF16)
            ra[rows, pl.ds(v_col, width)] = dot(xo[rows, x_part], weight(1, dim)).astype(BF16)

    w_loads[0].wait()
    w_loads[1].wait()
    project_kv(core)
    remote[0].wait()
    project_kv(1 - core)

    def head(h, column=0):
        return pl.ds(column + h * HEAD_DIM, HEAD_DIM)

    def accumulate(left, right, slot, total, reverse):
        total[...] = jnp.zeros_like(total)

        @pl.loop(0, n_blocks // 2)
        def _(step):
            for inner in range(2):
                block = (n_blocks - 1 - 2 * step - inner) if reverse else 2 * step + inner
                rows = aligned(block, BLOCK_LEN)
                for h in range(n_heads):
                    running = total[h]
                    grads[slot + block, :, head(h)] = running
                    total[h] = running + dot_t(left(rows, h), right(rows, h))

    def q_of(rows, h):
        return q[rows, head(h)]

    def do_of(rows, h):
        return do[rows, head(h)]

    def k_of(rows, h):
        return ra[rows, head(h, k_col)]

    def v_of(rows, h):
        return ra[rows, head(h, v_col)]

    def chain_copy(which, h):
        src, dst, target = ((s_out, s_in, up), (r_out, r_in, down))[which]
        return send(src.at[h], dst.at[h], chain_sems.at[which, 0, h], chain_sems.at[which, 1, h], target)

    def chain_step(which, h):
        first, last = ((0, n_chips - 1), (n_chips - 1, 0))[which]
        src, dst = ((s_out, s_in), (r_out, r_in))[which]

        @pl.when(chip == first)
        def _():
            dst[h] = jnp.zeros_like(dst[h])

        @pl.when(chip != first)
        def _():
            chain_copy(which, h).wait_recv()
            src[h] = src[h] + dst[h]

        @pl.when(chip != last)
        def _():
            chain_copy(which, h).start()

    def chain_s(tick):
        @pl.when((tick >= 3 * chip) & (tick < 3 * chip + n_heads))
        def _():
            chain_step(0, tick - 3 * chip)

    accumulate(k_of, v_of, kv_slot, s_out, False)

    def project_qdo(half, first_tick):
        @pl.loop(0, steps)
        def _(step):
            chain_s(first_tick + 2 * step)
            chain_s(first_tick + 2 * step + 1)
            rows = part_rows(half, step)
            q[rows, :] = dot(xo[rows, x_part], weight(2, dim)).astype(BF16)
            product = dot_nt(ra[rows, pl.ds(width, width)], weight(6, width))
            product += dot_nt(ra[rows, pl.ds(2 * width, width)], weight(7, width))
            do[rows, :] = product.astype(BF16)

    for load in w_loads[2:]:
        load.wait()
    project_qdo(core, 0)
    remote[1].wait()
    project_qdo(1 - core, 2 * steps)

    causal = lax.broadcasted_iota(jnp.int32, (BLOCK_LEN, BLOCK_LEN), 0) >= lax.broadcasted_iota(jnp.int32, (BLOCK_LEN, BLOCK_LEN), 1)

    def block_scores(block):
        rows = aligned(block, BLOCK_LEN)
        a_rows = pl.ds(pl.multiple_of(a_row + block * BLOCK_LEN, BLOCK_LEN), BLOCK_LEN)
        b_rows = pl.ds(pl.multiple_of(b_row + block * BLOCK_LEN, BLOCK_LEN), BLOCK_LEN)
        for h in range(n_heads):
            w_s[a_rows, head(h)] = jnp.where(causal, dot_nt(q_of(rows, h), k_of(rows, h)), 0.0).astype(BF16)
            w_s[b_rows, head(h)] = jnp.where(causal, dot_nt(do_of(rows, h), v_of(rows, h)), 0.0).astype(BF16)

    @pl.loop(0, max(3 * (n_chips - 1) + n_heads - 4 * steps, n_blocks // 2))
    def _(step):
        chain_s(4 * steps + step)

        @pl.when(step < n_blocks // 2)
        def _():
            for inner in range(2):
                block_scores(2 * step + inner)

    def scores(block, h):
        a_rows = pl.ds(pl.multiple_of(a_row + block * BLOCK_LEN, BLOCK_LEN), BLOCK_LEN)
        b_rows = pl.ds(pl.multiple_of(b_row + block * BLOCK_LEN, BLOCK_LEN), BLOCK_LEN)
        return w_s[a_rows, head(h)], w_s[b_rows, head(h)]

    def both(left, right, top, bottom):
        out = dot(jnp.concatenate([left, right], axis=1), jnp.concatenate([top, bottom], axis=0))
        return (out * scale).astype(BF16)

    @pl.loop(0, n_blocks // 2)
    def _(step):
        for inner in range(2):
            block = 2 * step + inner
            rows = aligned(block, BLOCK_LEN)
            for h in range(n_heads):
                a, b = scores(block, h)
                s = (s_in[h] + grads[kv_slot + block, :, head(h)]).astype(BF16)
                xo[rows, head(h, dim)] = both(a, q_of(rows, h), v_of(rows, h), s)
                ra[rows, head(h)] = both(b, do_of(rows, h), k_of(rows, h), s.T)

    def rev_block(block):
        rows = aligned(block, BLOCK_LEN)
        for h in range(n_heads):
            a, b = scores(block, h)
            r = (r_in[h] + grads[qdo_slot + block, :, head(h)]).astype(BF16)
            dk = both(b.T, v_of(rows, h), q_of(rows, h), r.T)
            dv = both(a.T, k_of(rows, h), do_of(rows, h), r)
            ra[rows, head(h, k_col)] = dk
            ra[rows, head(h, v_col)] = dv

    def credit(which):
        pl.semaphore_signal(credits.at[which], inc=1, device_id={"sp": previous}, device_id_type=MESH)

    def term(late, unit):
        inside, second = lax.rem(unit, per_weight), lax.div(unit, per_weight)
        if late:
            left, right = inside, 3 + second
        else:
            left = (1 - second) * inside + second * (per_weight + lax.div(inside, 2))
            right = second * (1 + lax.rem(inside, 2))
        return dot_t(xo[:, aligned(left, TILE)], ra[:, aligned(right, width)])

    def unit_of(step, piece):
        return lax.rem(rank - step + n_chips, n_chips) * early + piece

    def hop(late, step, piece):
        slot = grads.at[late * (n_slots // 2) + unit_of(step, piece)]
        sems = send_sems.at[late, step, piece], recv_sems.at[late, step, piece]
        return slot, sems

    def start_hop(late, step, piece, first):
        slot, sems = hop(late, step, piece)
        send(slot, land.at[late * early + piece] if first else slot, *sems, following).start()

    def run_ring(late, extra):
        offset = late * (n_slots // 2)

        @pl.loop(0, early)
        def _(piece):
            unit = unit_of(0, piece)
            grads[offset + unit] = term(late, unit)
            start_hop(late, 0, piece, True)

        @pl.loop(0, (n_chips - 1) * early)
        def _(index):
            step, piece = lax.div(index, early) + 1, lax.rem(index, early)
            unit = unit_of(step, piece)
            slot = offset + unit
            extra(index)
            mine = term(late, unit)

            @pl.when(step == 1)
            def _():
                place = land.at[late * early + piece]
                send(place, place, send_sems.at[late, 0, piece], recv_sems.at[late, 0, piece], following).wait_recv()
                grads[slot] = place[...] + mine

            @pl.when(step > 1)
            def _():
                place = grads.at[slot]
                send(place, place, send_sems.at[late, step - 1, piece], recv_sems.at[late, step - 1, piece], following).wait_recv()
                grads[slot] = grads[slot] + mine

            @pl.when(index == 0)
            def _():
                pl.semaphore_wait(credits.at[late], 1)

            @pl.when(step < n_chips - 1)
            def _():
                start_hop(late, step, piece, False)

            @pl.when(step == n_chips - 1)
            def _():
                pltpu.make_async_copy(grads.at[slot], red_out.at[late * early + piece], red_sems.at[late * early + piece]).start()

    share = n_blocks // 4

    def reverse_work(index):
        @pl.when(index == 0)
        def _():
            accumulate(q_of, do_of, qdo_slot, r_out, True)

        @pl.when(index == n_chips - chip)
        def _():
            for h in range(n_heads):
                chain_step(1, h)

        @pl.when((index > n_chips) & (index <= n_chips + 4))
        def _():
            @pl.loop(0, share)
            def _(part):
                rev_block((index - n_chips - 1) * share + part)

        @pl.when(index == n_chips + 4)
        def _():
            credit(1)

    credit(0)
    run_ring(0, reverse_work)

    copies = []
    for index, (src, column) in enumerate(((xo, dim), (ra, 0), (ra, k_col), (ra, v_col))):
        part = pl.ds(column, width)
        copies.append(pltpu.make_async_copy(src.at[own_rows, part], own_out.at[index, :, w_cols], own_sems.at[index, 0]))
        copies.append(send(src.at[peer_rows, part], own_out.at[index, :, w_cols], own_sems.at[index, 1], own_sems.at[index, 2], peer))
    for copy in copies:
        copy.start()

    run_ring(1, lambda index: None)

    for which, last in ((0, n_chips - 1), (1, 0)):
        @pl.when(chip != last)
        def _():
            for h in range(n_heads):
                chain_copy(which, h).wait_send()

    for late in range(2):
        @pl.loop(0, (n_chips - 1) * early)
        def _(index):
            step, piece = lax.div(index, early), lax.rem(index, early)
            slot, sems = hop(late, step, piece)
            send(slot, slot, *sems, following).wait_send()

    for copy in copies:
        copy.wait()
    for late in range(2):
        for piece in range(early):
            slot = late * (n_slots // 2) + lax.rem(rank + 1, n_chips) * early + piece
            pltpu.make_async_copy(grads.at[slot], red_out.at[late * early + piece], red_sems.at[late * early + piece]).wait()


def tile_slot(chunk, piece, early):
    return chunk * early + lax.rem(piece, early), lax.div(piece, early)


def gather_kernel(n_seq, red, own, wq, wk, wv, wo, rows_out, both_out, own_s, wo_s, w_s, own_sems, w_sems, send_sems, recv_sems, peer_sems):
    core, rank, n_chips, peer, following, previous = ring(n_seq)
    mine_out, peer_out = both_out.at[0], both_out.at[1]
    y_out, dx_out = rows_out.at[0], rows_out.at[1]
    n_slots, _, width = mine_out.shape
    dim = 2 * width
    early = 2 * (dim // TILE) // n_chips
    pieces = 2 * early
    n_rows = own.shape[1]
    unit_cols = wo_s.shape[2]
    n_units = dim // unit_cols
    row_blocks = n_rows // ROWS

    def slot_of(chunk, piece):
        unit, late = tile_slot(chunk, piece, early)
        return unit + late * (n_slots // 2)

    def held(step, piece):
        return slot_of(lax.rem(rank + 1 - step + n_chips, n_chips), piece)

    def w_loads(unit, buffer):
        part = aligned(unit, unit_cols)
        loads = [pltpu.make_async_copy(wo.at[:, part], wo_s.at[buffer], w_sems.at[buffer, 0])]
        for index, weight in enumerate((wq, wk, wv)):
            loads.append(pltpu.make_async_copy(weight.at[part], w_s.at[buffer, index], w_sems.at[buffer, 1 + index]))
        return loads

    own_load = pltpu.make_async_copy(own, own_s, own_sems.at[0])
    own_load.start()
    for unit in range(2):
        for load in w_loads(unit, unit):
            load.start()
    red_loads = [pltpu.make_async_copy(red.at[piece], mine_out.at[held(0, piece)], own_sems.at[1 + piece]) for piece in range(pieces)]
    for load in red_loads:
        load.start()

    entry_barrier((peer, following, previous))

    def to_next(step, piece):
        slot = held(step, piece)
        return send(mine_out.at[slot], mine_out.at[slot], send_sems.at[step, piece], recv_sems.at[step, piece], following)

    def arrival(step, piece):
        slot = held(step + 1, piece)
        return send(mine_out.at[slot], mine_out.at[slot], send_sems.at[step, piece], recv_sems.at[step, piece], following)

    def to_peer(step, piece):
        slot = held(step, piece)
        return send(mine_out.at[slot], peer_out.at[slot], peer_sems.at[0, step, piece], peer_sems.at[1, step, piece], peer)

    for piece in range(pieces):
        red_loads[piece].wait()
        to_next(0, piece).start()
        to_peer(0, piece).start()
    own_load.wait()

    def project(unit, block):
        buffer = lax.rem(unit, 2)

        @pl.when(block == 0)
        def _():
            for load in w_loads(unit, buffer):
                load.wait()

        rows, cols = aligned(block, ROWS), aligned(unit, unit_cols)
        y_out[rows, cols] = dot(own_s[0, rows, :], wo_s[buffer]).astype(BF16)
        total = dot_nt(own_s[1, rows, :], w_s[buffer, 0])
        total += dot_nt(own_s[2, rows, :], w_s[buffer, 1])
        total += dot_nt(own_s[3, rows, :], w_s[buffer, 2])
        dx_out[rows, cols] = total.astype(BF16)

        @pl.when((block == row_blocks - 1) & (unit + 2 < n_units))
        def _():
            for load in w_loads(unit + 2, buffer):
                load.start()

    @pl.loop(0, (n_chips - 1) * pieces)
    def _(index):
        step, piece = lax.div(index, pieces), lax.rem(index, pieces)

        @pl.when(index < n_units * row_blocks)
        def _():
            project(lax.div(index, row_blocks), lax.rem(index, row_blocks))

        arrival(step, piece).wait_recv()

        @pl.when(step < n_chips - 2)
        def _():
            to_next(step + 1, piece).start()

        to_peer(step + 1, piece).start()

    @pl.loop(0, n_chips * pieces)
    def _(index):
        step, piece = lax.div(index, pieces), lax.rem(index, pieces)

        @pl.when(step < n_chips - 1)
        def _():
            to_next(step, piece).wait_send()

        to_peer(step, piece).wait()


def place_kernel(results, both, y, dx, gq, gk, gv, go, sems):
    core = lax.rem(lax.axis_index("sp"), 2)
    _, n_slots, _, width = both.shape
    per_weight = n_slots // 4
    copies = [pltpu.make_async_copy(results.at[0], y, sems.at[2]), pltpu.make_async_copy(results.at[1], dx, sems.at[3])]
    for side, half in enumerate((core, 1 - core)):
        cols = aligned(half, width)
        for slot in range(n_slots):
            weight, inside = slot // per_weight, slot % per_weight
            if weight == 1:
                rows = pl.ds(pl.multiple_of(half * width + inside // 2 * TILE, TILE), TILE)
                dst = go.at[rows, pl.ds(inside % 2 * width, width)]
            else:
                dst = (gq, None, gk, gv)[weight].at[pl.ds(inside * TILE, TILE), cols]
            copies.append(pltpu.make_async_copy(both.at[side, slot], dst, sems.at[side]))
    for copy in copies:
        copy.start()
    for copy in copies:
        copy.wait()


def solution(mesh):
    n_seq = mesh.shape["sp"]
    n_chips = n_seq // 2
    row_spec = P(("dp", "sp"), None)
    grad_spec = P("dp", None)
    any_spec = pl.BlockSpec(memory_space=pl.ANY)
    vmem_spec = pl.BlockSpec(memory_space=pltpu.VMEM)
    dma = pltpu.SemaphoreType.DMA

    def params(collective_id, limit=VMEM_LIMIT):
        return pltpu.CompilerParams(collective_id=collective_id, has_side_effects=True, vmem_limit_bytes=limit)

    def local_layer(tokens, w_q, w_k, w_v, w_o, grad_y):
        n_rows, dim = tokens.shape
        width = dim // 2
        n_heads = width // HEAD_DIM
        rows = 2 * n_rows
        n_slots = 4 * (dim // TILE)
        pieces = n_slots // n_chips
        scale = 1.0 / math.sqrt(n_rows * n_seq * HEAD_DIM)
        state = (n_heads, HEAD_DIM, HEAD_DIM)

        red, own = pl.pallas_call(
            functools.partial(attention_kernel, n_seq, scale),
            out_shape=(jax.ShapeDtypeStruct((pieces, TILE, width), F32), jax.ShapeDtypeStruct((4, n_rows, dim), BF16)),
            in_specs=[any_spec] * 6,
            out_specs=(any_spec,) * 2,
            scratch_shapes=[pltpu.VMEM((rows, dim + width), BF16), pltpu.VMEM((rows, dim + 3 * width), BF16), pltpu.VMEM((4 * dim, width), BF16)]
            + [pltpu.VMEM((rows, width), BF16)] * 2
            + [pltpu.VMEM((n_slots, TILE, width), F32), pltpu.VMEM((pieces, TILE, width), F32)]
            + [pltpu.VMEM(state, F32)] * 4
            + [dma((2, 3)), dma((5,)), dma((2, 2, n_heads))]
            + [dma((2, n_chips - 1, pieces // 2))] * 2
            + [dma((4, 3)), dma((pieces,)), pltpu.SemaphoreType.REGULAR((2,))],
            compiler_params=params(0),
            name="attention",
        )(tokens, grad_y, w_q, w_k, w_v, w_o)

        unit_cols = min(256, dim // 2)
        halves = (2, n_slots, TILE, width)
        room = VMEM_LIMIT - math.prod(halves) * 4 - 4 * n_rows * dim - (1 << 20)
        results = pl.pallas_call(
            functools.partial(gather_kernel, n_seq),
            out_shape=(pltpu.VMEM((2, n_rows, dim), BF16), pltpu.VMEM(halves, F32)),
            in_specs=[any_spec] * 6,
            out_specs=(vmem_spec,) * 2,
            scratch_shapes=[pltpu.VMEM((4, n_rows, dim), BF16), pltpu.VMEM((2, dim, unit_cols), BF16), pltpu.VMEM((2, 3, unit_cols, dim), BF16)]
            + [dma((1 + pieces,)), dma((2, 4)), dma((n_chips - 1, pieces)), dma((n_chips - 1, pieces)), dma((2, n_chips, pieces))],
            compiler_params=params(1, room),
            name="gather",
        )(red, own, w_q, w_k, w_v, w_o)

        return pl.pallas_call(
            place_kernel,
            out_shape=(jax.ShapeDtypeStruct((n_rows, dim), BF16),) * 2 + (jax.ShapeDtypeStruct((dim, dim), F32),) * 4,
            in_specs=[vmem_spec] * 2,
            out_specs=(any_spec,) * 6,
            scratch_shapes=[dma((4,))],
            compiler_params=pltpu.CompilerParams(vmem_limit_bytes=1 << 20),
            name="place",
        )(*results)

    return jax.shard_map(local_layer, mesh=mesh, in_specs=(row_spec, P(), P(), P(), P(), row_spec), out_specs=(row_spec, row_spec, grad_spec, grad_spec, grad_spec, grad_spec), check_vma=False)
```

```python
import functools
import math
import jax
import jax.numpy as jnp
from jax import lax
from jax.experimental import pallas as pl
from jax.experimental.pallas import tpu as pltpu
from jax.sharding import PartitionSpec as P

HEAD_DIM = 128
BLOCK_LEN = 128
TILE = 128
ROWS = 256
PROJECT_ROWS = 512
MESH = pl.DeviceIdType.MESH
VMEM_LIMIT = 67_043_328
F32 = jnp.float32
BF16 = jnp.bfloat16


def dot_t(lhs, rhs):
    return lax.dot_general(lhs, rhs, (((0,), (0,)), ((), ())), preferred_element_type=F32)


def dot_nt(lhs, rhs):
    return lax.dot_general(lhs, rhs, (((1,), (1,)), ((), ())), preferred_element_type=F32)


def dot(lhs, rhs):
    return jnp.dot(lhs, rhs, preferred_element_type=F32)


def aligned(index, size):
    return pl.ds(pl.multiple_of(index * size, size), size)


def position(n_seq):
    me = lax.axis_index("sp")
    core, chip = lax.rem(me, 2), lax.div(me, 2)
    return core, chip, n_seq // 2, me + 1 - 2 * core


def send(src, dst, send_sem, recv_sem, target):
    return pltpu.make_async_remote_copy(src_ref=src, dst_ref=dst, send_sem=send_sem, recv_sem=recv_sem, device_id={"sp": target}, device_id_type=MESH)


def entry_barrier(targets):
    barrier = pltpu.get_barrier_semaphore()
    for target in targets:
        pl.semaphore_signal(barrier, inc=1, device_id={"sp": target}, device_id_type=MESH)
    pl.semaphore_wait(barrier, len(targets))


def ring(n_seq):
    core, chip, n_chips, peer = position(n_seq)
    me = lax.axis_index("sp")
    rank = (1 - core) * chip + core * lax.rem(n_chips - chip, n_chips)
    following = lax.rem(me + 2 - 4 * core + n_seq, n_seq)
    previous = lax.rem(me - 2 + 4 * core + n_seq, n_seq)
    return core, rank, n_chips, peer, following, previous


def attention_kernel(n_seq, scale, x, dy, wq, wk, wv, wo, red_out, own_out, xo, ra, w_s, q, do, grads, land, s_in, s_out, r_in, r_out, x_sems, w_sems, chain_sems, send_sems, recv_sems, own_sems, red_sems, credits):
    _, chip, _, _ = position(n_seq)
    core, rank, n_chips, peer, following, previous = ring(n_seq)
    me = lax.axis_index("sp")
    up, down = lax.rem(me + 2, n_seq), lax.rem(me + n_seq - 2, n_seq)
    n_rows, dim = x.shape
    all_rows, width = q.shape
    n_heads = width // HEAD_DIM
    n_blocks = all_rows // BLOCK_LEN
    n_slots = grads.shape[0]
    per_weight = dim // TILE
    early = 2 * per_weight // n_chips
    own_rows, peer_rows = aligned(core, n_rows), aligned(1 - core, n_rows)
    w_cols = aligned(core, width)
    k_col, v_col, a_row, b_row = width + dim, 2 * width + dim, 0, all_rows
    kv_slot, qdo_slot = 0, n_slots // 2

    x_part, dy_part = pl.ds(0, dim), pl.ds(width, dim)
    local, remote = [], []
    for index, (src, dst) in enumerate(((x, xo.at[own_rows, x_part]), (dy, ra.at[own_rows, dy_part]))):
        local.append(pltpu.make_async_copy(src, dst, x_sems.at[index, 2]))
        remote.append(send(dst, dst, x_sems.at[index, 0], x_sems.at[index, 1], peer))
    w_loads = [pltpu.make_async_copy(weight.at[:, w_cols], w_s.at[pl.ds(index * dim, dim)], w_sems.at[index]) for index, weight in enumerate((wk, wv, wq))]
    for part in range(2):
        w_loads.append(pltpu.make_async_copy(wo.at[w_cols, pl.ds(part * width, width)], w_s.at[pl.ds(3 * dim + part * width, width)], w_sems.at[3 + part]))
    local[0].start()
    for load in w_loads[:2]:
        load.start()
    local[1].start()
    for load in w_loads[2:]:
        load.start()
    entry_barrier((peer, up, down))
    for index in range(2):
        local[index].wait()
        remote[index].start()

    def weight(index, size):
        return w_s[pl.ds(index * size, size), :]

    part_len = min(PROJECT_ROWS, n_rows)
    steps = n_rows // part_len

    def part_rows(half, step):
        return pl.ds(pl.multiple_of(half * n_rows + step * part_len, part_len), part_len)

    def project_kv(half):
        @pl.loop(0, steps)
        def _(step):
            rows = part_rows(half, step)
            ra[rows, pl.ds(k_col, width)] = dot(xo[rows, x_part], weight(0, dim)).astype(BF16)
            ra[rows, pl.ds(v_col, width)] = dot(xo[rows, x_part], weight(1, dim)).astype(BF16)

    w_loads[0].wait()
    w_loads[1].wait()
    project_kv(core)
    remote[0].wait()
    project_kv(1 - core)

    def head(h, column=0):
        return pl.ds(column + h * HEAD_DIM, HEAD_DIM)

    def accumulate(left, right, slot, total, reverse):
        total[...] = jnp.zeros_like(total)

        @pl.loop(0, n_blocks // 2)
        def _(step):
            for inner in range(2):
                block = (n_blocks - 1 - 2 * step - inner) if reverse else 2 * step + inner
                rows = aligned(block, BLOCK_LEN)
                for h in range(n_heads):
                    running = total[h]
                    grads[slot + block, :, head(h)] = running
                    total[h] = running + dot_t(left(rows, h), right(rows, h))

    def q_of(rows, h):
        return q[rows, head(h)]

    def do_of(rows, h):
        return do[rows, head(h)]

    def k_of(rows, h):
        return ra[rows, head(h, k_col)]

    def v_of(rows, h):
        return ra[rows, head(h, v_col)]

    def chain_copy(which, h):
        src, dst, target = ((s_out, s_in, up), (r_out, r_in, down))[which]
        return send(src.at[h], dst.at[h], chain_sems.at[which, 0, h], chain_sems.at[which, 1, h], target)

    def chain_step(which, h):
        first, last = ((0, n_chips - 1), (n_chips - 1, 0))[which]
        src, dst = ((s_out, s_in), (r_out, r_in))[which]

        @pl.when(chip == first)
        def _():
            dst[h] = jnp.zeros_like(dst[h])

        @pl.when(chip != first)
        def _():
            chain_copy(which, h).wait_recv()
            src[h] = src[h] + dst[h]

        @pl.when(chip != last)
        def _():
            chain_copy(which, h).start()

    def chain_s(tick):
        @pl.when((tick >= 3 * chip) & (tick < 3 * chip + n_heads))
        def _():
            chain_step(0, tick - 3 * chip)

    accumulate(k_of, v_of, kv_slot, s_out, False)

    def project_qdo(half, first_tick):
        @pl.loop(0, steps)
        def _(step):
            chain_s(first_tick + 2 * step)
            chain_s(first_tick + 2 * step + 1)
            rows = part_rows(half, step)
            q[rows, :] = dot(xo[rows, x_part], weight(2, dim)).astype(BF16)
            product = dot_nt(ra[rows, pl.ds(width, width)], weight(6, width))
            product += dot_nt(ra[rows, pl.ds(2 * width, width)], weight(7, width))
            do[rows, :] = product.astype(BF16)

    for load in w_loads[2:]:
        load.wait()
    project_qdo(core, 0)
    remote[1].wait()
    project_qdo(1 - core, 2 * steps)

    causal = lax.broadcasted_iota(jnp.int32, (BLOCK_LEN, BLOCK_LEN), 0) >= lax.broadcasted_iota(jnp.int32, (BLOCK_LEN, BLOCK_LEN), 1)

    def block_scores(block):
        rows = aligned(block, BLOCK_LEN)
        a_rows = pl.ds(pl.multiple_of(a_row + block * BLOCK_LEN, BLOCK_LEN), BLOCK_LEN)
        b_rows = pl.ds(pl.multiple_of(b_row + block * BLOCK_LEN, BLOCK_LEN), BLOCK_LEN)
        for h in range(n_heads):
            w_s[a_rows, head(h)] = jnp.where(causal, dot_nt(q_of(rows, h), k_of(rows, h)), 0.0).astype(BF16)
            w_s[b_rows, head(h)] = jnp.where(causal, dot_nt(do_of(rows, h), v_of(rows, h)), 0.0).astype(BF16)

    @pl.loop(0, max(3 * (n_chips - 1) + n_heads - 4 * steps, n_blocks // 2))
    def _(step):
        chain_s(4 * steps + step)

        @pl.when(step < n_blocks // 2)
        def _():
            for inner in range(2):
                block_scores(2 * step + inner)

    def scores(block, h):
        a_rows = pl.ds(pl.multiple_of(a_row + block * BLOCK_LEN, BLOCK_LEN), BLOCK_LEN)
        b_rows = pl.ds(pl.multiple_of(b_row + block * BLOCK_LEN, BLOCK_LEN), BLOCK_LEN)
        return w_s[a_rows, head(h)], w_s[b_rows, head(h)]

    def both(left, right, top, bottom):
        out = dot(jnp.concatenate([left, right], axis=1), jnp.concatenate([top, bottom], axis=0))
        return (out * scale).astype(BF16)

    @pl.loop(0, n_blocks // 2)
    def _(step):
        for inner in range(2):
            block = 2 * step + inner
            rows = aligned(block, BLOCK_LEN)
            for h in range(n_heads):
                a, b = scores(block, h)
                s = (s_in[h] + grads[kv_slot + block, :, head(h)]).astype(BF16)
                xo[rows, head(h, dim)] = both(a, q_of(rows, h), v_of(rows, h), s)
                ra[rows, head(h)] = both(b, do_of(rows, h), k_of(rows, h), s.T)

    def rev_block(block):
        rows = aligned(block, BLOCK_LEN)
        for h in range(n_heads):
            a, b = scores(block, h)
            r = (r_in[h] + grads[qdo_slot + block, :, head(h)]).astype(BF16)
            dk = both(b.T, v_of(rows, h), q_of(rows, h), r.T)
            dv = both(a.T, k_of(rows, h), do_of(rows, h), r)
            ra[rows, head(h, k_col)] = dk
            ra[rows, head(h, v_col)] = dv

    def credit(which):
        pl.semaphore_signal(credits.at[which], inc=1, device_id={"sp": previous}, device_id_type=MESH)

    def term(late, unit):
        inside, second = lax.rem(unit, per_weight), lax.div(unit, per_weight)
        if late:
            left, right = inside, 3 + second
        else:
            left = (1 - second) * inside + second * (per_weight + lax.div(inside, 2))
            right = second * (1 + lax.rem(inside, 2))
        return dot_t(xo[:, aligned(left, TILE)], ra[:, aligned(right, width)])

    def unit_of(step, piece):
        return lax.rem(rank - step + n_chips, n_chips) * early + piece

    def hop(late, step, piece):
        slot = grads.at[late * (n_slots // 2) + unit_of(step, piece)]
        sems = send_sems.at[late, step, piece], recv_sems.at[late, step, piece]
        return slot, sems

    def start_hop(late, step, piece, first):
        slot, sems = hop(late, step, piece)
        send(slot, land.at[late * early + piece] if first else slot, *sems, following).start()

    def start_ring(late):
        @pl.loop(0, early)
        def _(piece):
            unit = unit_of(0, piece)
            grads[late * (n_slots // 2) + unit] = term(late, unit)
            start_hop(late, 0, piece, True)

    def run_ring(late, extra):
        offset = late * (n_slots // 2)

        @pl.loop(0, (n_chips - 1) * early)
        def _(index):
            step, piece = lax.div(index, early) + 1, lax.rem(index, early)
            unit = unit_of(step, piece)
            slot = offset + unit
            extra(index)
            mine = term(late, unit)

            @pl.when(step == 1)
            def _():
                place = land.at[late * early + piece]
                send(place, place, send_sems.at[late, 0, piece], recv_sems.at[late, 0, piece], following).wait_recv()
                grads[slot] = place[...] + mine

            @pl.when(step > 1)
            def _():
                place = grads.at[slot]
                send(place, place, send_sems.at[late, step - 1, piece], recv_sems.at[late, step - 1, piece], following).wait_recv()
                grads[slot] = grads[slot] + mine

            @pl.when(index == 0)
            def _():
                pl.semaphore_wait(credits.at[late], 1)

            @pl.when(step < n_chips - 1)
            def _():
                start_hop(late, step, piece, False)

            @pl.when(step == n_chips - 1)
            def _():
                pltpu.make_async_copy(grads.at[slot], red_out.at[late * early + piece], red_sems.at[late * early + piece]).start()

    share = n_blocks // 4

    def reverse_work(index):
        @pl.when(index == 0)
        def _():
            accumulate(q_of, do_of, qdo_slot, r_out, True)

        @pl.when(index == n_chips - chip)
        def _():
            for h in range(n_heads):
                chain_step(1, h)

        @pl.when((index > n_chips) & (index <= n_chips + 4))
        def _():
            @pl.loop(0, share)
            def _(part):
                rev_block((index - n_chips - 1) * share + part)

        @pl.when(index == n_chips + 4)
        def _():
            credit(1)

        @pl.when(index == (n_chips - 2) * early)
        def _():
            start_ring(1)

    credit(0)
    start_ring(0)
    run_ring(0, reverse_work)

    copies = []
    for index, (src, column) in enumerate(((xo, dim), (ra, 0), (ra, k_col), (ra, v_col))):
        part = pl.ds(column, width)
        copies.append(pltpu.make_async_copy(src.at[own_rows, part], own_out.at[index, :, w_cols], own_sems.at[index, 0]))
        copies.append(send(src.at[peer_rows, part], own_out.at[index, :, w_cols], own_sems.at[index, 1], own_sems.at[index, 2], peer))
    for copy in copies:
        copy.start()

    run_ring(1, lambda index: None)

    for which, last in ((0, n_chips - 1), (1, 0)):
        @pl.when(chip != last)
        def _():
            for h in range(n_heads):
                chain_copy(which, h).wait_send()

    for late in range(2):
        @pl.loop(0, (n_chips - 1) * early)
        def _(index):
            step, piece = lax.div(index, early), lax.rem(index, early)
            slot, sems = hop(late, step, piece)
            send(slot, slot, *sems, following).wait_send()

    for copy in copies:
        copy.wait()
    for late in range(2):
        for piece in range(early):
            slot = late * (n_slots // 2) + lax.rem(rank + 1, n_chips) * early + piece
            pltpu.make_async_copy(grads.at[slot], red_out.at[late * early + piece], red_sems.at[late * early + piece]).wait()


def tile_slot(chunk, piece, early):
    return chunk * early + lax.rem(piece, early), lax.div(piece, early)


def gather_kernel(n_seq, red, own, wq, wk, wv, wo, rows_out, both_out, own_s, wo_s, w_s, own_sems, w_sems, send_sems, recv_sems, peer_sems):
    core, rank, n_chips, peer, following, previous = ring(n_seq)
    mine_out, peer_out = both_out.at[0], both_out.at[1]
    y_out, dx_out = rows_out.at[0], rows_out.at[1]
    n_slots, _, width = mine_out.shape
    dim = 2 * width
    early = 2 * (dim // TILE) // n_chips
    pieces = 2 * early
    n_rows = own.shape[1]
    unit_cols = wo_s.shape[2]
    n_units = dim // unit_cols
    row_blocks = n_rows // ROWS

    def slot_of(chunk, piece):
        unit, late = tile_slot(chunk, piece, early)
        return unit + late * (n_slots // 2)

    def held(step, piece):
        return slot_of(lax.rem(rank + 1 - step + n_chips, n_chips), piece)

    def w_loads(unit, buffer):
        part = aligned(unit, unit_cols)
        loads = [pltpu.make_async_copy(wo.at[:, part], wo_s.at[buffer], w_sems.at[buffer, 0])]
        for index, weight in enumerate((wq, wk, wv)):
            loads.append(pltpu.make_async_copy(weight.at[part], w_s.at[buffer, index], w_sems.at[buffer, 1 + index]))
        return loads

    own_load = pltpu.make_async_copy(own, own_s, own_sems.at[0])
    own_load.start()
    for unit in range(2):
        for load in w_loads(unit, unit):
            load.start()
    red_loads = [pltpu.make_async_copy(red.at[piece], mine_out.at[held(0, piece)], own_sems.at[1 + piece]) for piece in range(pieces)]
    for load in red_loads:
        load.start()

    entry_barrier((peer, following, previous))

    def to_next(step, piece):
        slot = held(step, piece)
        return send(mine_out.at[slot], mine_out.at[slot], send_sems.at[step, piece], recv_sems.at[step, piece], following)

    def arrival(step, piece):
        slot = held(step + 1, piece)
        return send(mine_out.at[slot], mine_out.at[slot], send_sems.at[step, piece], recv_sems.at[step, piece], following)

    def to_peer(step, piece):
        slot = held(step, piece)
        return send(mine_out.at[slot], peer_out.at[slot], peer_sems.at[0, step, piece], peer_sems.at[1, step, piece], peer)

    for piece in range(pieces):
        red_loads[piece].wait()
        to_next(0, piece).start()
        to_peer(0, piece).start()
    own_load.wait()

    def project(unit, block):
        buffer = lax.rem(unit, 2)

        @pl.when(block == 0)
        def _():
            for load in w_loads(unit, buffer):
                load.wait()

        rows, cols = aligned(block, ROWS), aligned(unit, unit_cols)
        y_out[rows, cols] = dot(own_s[0, rows, :], wo_s[buffer]).astype(BF16)
        total = dot_nt(own_s[1, rows, :], w_s[buffer, 0])
        total += dot_nt(own_s[2, rows, :], w_s[buffer, 1])
        total += dot_nt(own_s[3, rows, :], w_s[buffer, 2])
        dx_out[rows, cols] = total.astype(BF16)

        @pl.when((block == row_blocks - 1) & (unit + 2 < n_units))
        def _():
            for load in w_loads(unit + 2, buffer):
                load.start()

    @pl.loop(0, (n_chips - 1) * pieces)
    def _(index):
        step, piece = lax.div(index, pieces), lax.rem(index, pieces)

        @pl.when(index < n_units * row_blocks)
        def _():
            project(lax.div(index, row_blocks), lax.rem(index, row_blocks))

        arrival(step, piece).wait_recv()

        @pl.when(step < n_chips - 2)
        def _():
            to_next(step + 1, piece).start()

        to_peer(step + 1, piece).start()

    @pl.loop(0, n_chips * pieces)
    def _(index):
        step, piece = lax.div(index, pieces), lax.rem(index, pieces)

        @pl.when(step < n_chips - 1)
        def _():
            to_next(step, piece).wait_send()

        to_peer(step, piece).wait()


def place_kernel(results, both, y, dx, gq, gk, gv, go, sems):
    core = lax.rem(lax.axis_index("sp"), 2)
    _, n_slots, _, width = both.shape
    per_weight = n_slots // 4
    copies = [pltpu.make_async_copy(results.at[0], y, sems.at[2]), pltpu.make_async_copy(results.at[1], dx, sems.at[3])]
    for side, half in enumerate((core, 1 - core)):
        cols = aligned(half, width)
        for slot in range(n_slots):
            weight, inside = slot // per_weight, slot % per_weight
            if weight == 1:
                rows = pl.ds(pl.multiple_of(half * width + inside // 2 * TILE, TILE), TILE)
                dst = go.at[rows, pl.ds(inside % 2 * width, width)]
            else:
                dst = (gq, None, gk, gv)[weight].at[pl.ds(inside * TILE, TILE), cols]
            copies.append(pltpu.make_async_copy(both.at[side, slot], dst, sems.at[side]))
    for copy in copies:
        copy.start()
    for copy in copies:
        copy.wait()


def solution(mesh):
    n_seq = mesh.shape["sp"]
    n_chips = n_seq // 2
    row_spec = P(("dp", "sp"), None)
    grad_spec = P("dp", None)
    any_spec = pl.BlockSpec(memory_space=pl.ANY)
    vmem_spec = pl.BlockSpec(memory_space=pltpu.VMEM)
    dma = pltpu.SemaphoreType.DMA

    def params(collective_id, limit=VMEM_LIMIT):
        return pltpu.CompilerParams(collective_id=collective_id, has_side_effects=True, vmem_limit_bytes=limit)

    def local_layer(tokens, w_q, w_k, w_v, w_o, grad_y):
        n_rows, dim = tokens.shape
        width = dim // 2
        n_heads = width // HEAD_DIM
        rows = 2 * n_rows
        n_slots = 4 * (dim // TILE)
        pieces = n_slots // n_chips
        scale = 1.0 / math.sqrt(n_rows * n_seq * HEAD_DIM)
        state = (n_heads, HEAD_DIM, HEAD_DIM)

        red, own = pl.pallas_call(
            functools.partial(attention_kernel, n_seq, scale),
            out_shape=(jax.ShapeDtypeStruct((pieces, TILE, width), F32), jax.ShapeDtypeStruct((4, n_rows, dim), BF16)),
            in_specs=[any_spec] * 6,
            out_specs=(any_spec,) * 2,
            scratch_shapes=[pltpu.VMEM((rows, dim + width), BF16), pltpu.VMEM((rows, dim + 3 * width), BF16), pltpu.VMEM((4 * dim, width), BF16)]
            + [pltpu.VMEM((rows, width), BF16)] * 2
            + [pltpu.VMEM((n_slots, TILE, width), F32), pltpu.VMEM((pieces, TILE, width), F32)]
            + [pltpu.VMEM(state, F32)] * 4
            + [dma((2, 3)), dma((5,)), dma((2, 2, n_heads))]
            + [dma((2, n_chips - 1, pieces // 2))] * 2
            + [dma((4, 3)), dma((pieces,)), pltpu.SemaphoreType.REGULAR((2,))],
            compiler_params=params(0),
            name="attention",
        )(tokens, grad_y, w_q, w_k, w_v, w_o)

        unit_cols = min(256, dim // 2)
        halves = (2, n_slots, TILE, width)
        room = VMEM_LIMIT - math.prod(halves) * 4 - 4 * n_rows * dim - (1 << 20)
        results = pl.pallas_call(
            functools.partial(gather_kernel, n_seq),
            out_shape=(pltpu.VMEM((2, n_rows, dim), BF16), pltpu.VMEM(halves, F32)),
            in_specs=[any_spec] * 6,
            out_specs=(vmem_spec,) * 2,
            scratch_shapes=[pltpu.VMEM((4, n_rows, dim), BF16), pltpu.VMEM((2, dim, unit_cols), BF16), pltpu.VMEM((2, 3, unit_cols, dim), BF16)]
            + [dma((1 + pieces,)), dma((2, 4)), dma((n_chips - 1, pieces)), dma((n_chips - 1, pieces)), dma((2, n_chips, pieces))],
            compiler_params=params(1, room),
            name="gather",
        )(red, own, w_q, w_k, w_v, w_o)

        return pl.pallas_call(
            place_kernel,
            out_shape=(jax.ShapeDtypeStruct((n_rows, dim), BF16),) * 2 + (jax.ShapeDtypeStruct((dim, dim), F32),) * 4,
            in_specs=[vmem_spec] * 2,
            out_specs=(any_spec,) * 6,
            scratch_shapes=[dma((4,))],
            compiler_params=pltpu.CompilerParams(vmem_limit_bytes=1 << 20),
            name="place",
        )(*results)

    return jax.shard_map(local_layer, mesh=mesh, in_specs=(row_spec, P(), P(), P(), P(), row_spec), out_specs=(row_spec, row_spec, grad_spec, grad_spec, grad_spec, grad_spec), check_vma=False)
```
